32 devices in a mesh: snp: 8 (over z, y), probe: 4 (over x, core).
Axes of the slice: x: 2, y: 2, z: 4, core: 2. Of those that a mesh axis runs over, the one named last changes fastest.
Arguments:
- dosage: bfloat16 [256, 16384], P(None, 'snp'), may hold values from 0 to 2, as said below
- allele_freq: float32 [16384], P('snp'), may hold values from 0.05 to 0.5
- probes: bfloat16 [32, 256], P('probe'), may hold values from -1 to 1, as said below
Outputs:
- kin_twice: float32 [32, 256], P('probe', 'snp')
- forms: float32 [2, 32], P(None, 'probe')
- estimates: float32 [2], replicated
The draws below stay inside these ranges and needn't reach their ends.
Inputs may be any that keep to these rules, and one draw needn't show every extreme that they name: `dosage`: whole dosages. `probes`: every entry is -1 or 1.
All inputs are finite; a program needn't handle non-finite values.
Results may differ from the reference program's by a relative error of at most 0.0032.
Values may be sent and summed in bfloat16 or wider, within the bound.
No kernel may reach another device: no remote copies, remote signals or barrier semaphores. Data moves between devices by JAX's collectives and lax.ppermute only.
A program may use at most 64 MiB of HBM per device.

```python
import jax
import jax.numpy as jnp
from jax import lax

SNP_DEV = 2048
PROBES = 32
SNPS = 16384
SAMPLES = 256


def frequency_helper(key):
    return jax.random.uniform(jax.random.fold_in(key, 11), (SNPS,), jnp.float32, 0.05, 0.5)


def draw_allele_freq(key, part):
    return frequency_helper(key)


def draw_dosage(key, part):
    freq = frequency_helper(key)
    first_draw = jax.random.uniform(jax.random.fold_in(key, 21), (SAMPLES, SNPS), jnp.float32)
    copies = (first_draw < freq).astype(jnp.float32)
    second_draw = jax.random.uniform(jax.random.fold_in(key, 22), (SAMPLES, SNPS), jnp.float32)
    copies = copies + (second_draw < freq).astype(jnp.float32)
    return copies.astype(jnp.bfloat16)


def draw_probes(key, part):
    coins = jax.random.randint(jax.random.fold_in(key, 31), (PROBES, SAMPLES), 0, 2)
    return (2 * coins - 1).astype(jnp.float32).astype(jnp.bfloat16)


def setup_inputs(seed: int = 0) -> dict:
    key_list = jax.random.split(jax.random.key(seed), 4)
    return {
        "dosage": draw_dosage(jax.random.fold_in(key_list[3], 71), 0),
        "allele_freq": draw_allele_freq(jax.random.fold_in(key_list[3], 71), 0),
        "probes": draw_probes(jax.random.fold_in(key_list[3], 71), 0),
    }


def kinship_apply(vectors, dosage, allele_freq, width_blk):
    columns = dosage.shape[1]
    rows = dosage.shape[0]

    def column_step(column_step_index, running):
        start = (column_step_index * width_blk).astype(jnp.int32)
        dosage_blk = lax.dynamic_slice_in_dim(dosage, start, width_blk, 1)
        freq_blk = lax.dynamic_slice_in_dim(allele_freq, start, width_blk, 0)
        scaling = lax.rsqrt(2.0 * freq_blk * (1.0 - freq_blk))
        standard = ((dosage_blk.astype(jnp.float32) - 2.0 * freq_blk) * scaling).astype(jnp.bfloat16)
        projected = jnp.dot(vectors, standard, preferred_element_type=jnp.float32).astype(jnp.bfloat16)
        return running + lax.dot_general(projected, standard, (((1,), (1,)), ((), ())), preferred_element_type=jnp.float32)
    running = jnp.zeros((vectors.shape[0], rows), jnp.float32)
    running = lax.fori_loop(0, columns // width_blk, column_step, running)
    return running / columns

def reference(dosage, allele_freq, probes):
    kin_once = kinship_apply(probes, dosage, allele_freq, SNP_DEV)
    kin_twice = kinship_apply(kin_once.astype(jnp.bfloat16), dosage, allele_freq, SNP_DEV)
    signs = probes.astype(jnp.float32)
    count = dosage.shape[0]
    form_first = lax.optimization_barrier(jnp.sum(signs * kin_once, axis=1)) / count
    form_second = lax.optimization_barrier(jnp.sum(signs * kin_twice, axis=1)) / count
    forms = jnp.stack([form_first, form_second])
    estimates = lax.optimization_barrier(jnp.sum(forms, axis=1)) / probes.shape[0]
    return (kin_twice, forms, estimates)
```

```python
import jax
import jax.numpy as jnp
from jax import lax
from jax.sharding import PartitionSpec as P

BOTH = ("snp", "probe")


def body(dosage, allele_freq, probes):
    snp_count = lax.axis_size("snp")
    probe_count = lax.axis_size("probe")
    columns = dosage.shape[1] * snp_count
    samples = dosage.shape[0]
    rows = probes.shape[0]
    part = samples // (snp_count * probe_count)
    group = lax.axis_index("probe")
    scaling = lax.rsqrt(2.0 * allele_freq * (1.0 - allele_freq))
    standard = ((dosage.astype(jnp.float32) - 2.0 * allele_freq) * scaling).astype(jnp.bfloat16)
    across = (((1,), (1,)), ((), ()))
    mine = standard.reshape(snp_count, probe_count, part, -1)
    mine = lax.dynamic_index_in_dim(mine, group, 1, keepdims=False).reshape(snp_count * part, -1)
    projected = jnp.dot(probes, standard, preferred_element_type=jnp.float32).astype(jnp.bfloat16)
    left = jnp.concatenate([projected, mine], axis=0)
    partial = lax.dot_general(left, standard, across, preferred_element_type=jnp.float32) / columns
    signs = probes.astype(jnp.float32)
    signed = (signs * partial[:rows]).astype(jnp.bfloat16)
    kinship = partial[rows:].astype(jnp.bfloat16).reshape(snp_count, 1, part, samples)
    shape = (snp_count, probe_count)
    send = jnp.concatenate(
        [
            jnp.broadcast_to(signed, shape + (rows, samples)),
            jnp.broadcast_to(kinship, shape + (part, samples)),
        ],
        axis=2,
    ).reshape(snp_count * probe_count, rows + part, samples)
    got = lax.all_to_all(send, BOTH, 0, 0, tiled=True)
    summed = jnp.sum(got.reshape(shape + (rows + part, samples)).astype(jnp.float32), axis=0)
    signed_all = summed[:, :rows]
    kinship_owned = summed[:, rows:].reshape(probe_count * part, samples)
    rounded_all = lax.reduce_precision(signed_all, 8, 7)
    first = jnp.sum(signed_all, axis=2) / samples
    second = jnp.sum(rounded_all * signed_all, axis=2) / samples
    both = jnp.stack([first, second])
    estimates = jnp.sum(both, axis=(1, 2)) / (rows * probe_count)
    forms = lax.dynamic_index_in_dim(both, group, 1, keepdims=False)
    kin_round = signs * lax.dynamic_index_in_dim(rounded_all, group, 0, keepdims=False)
    kin_twice = lax.dot_general(
        kin_round, kinship_owned, across, precision=lax.Precision.HIGHEST,
        preferred_element_type=jnp.float32,
    )
    return (kin_twice, forms, estimates)


def solution(mesh):
    placed = (P(None, "snp"), P("snp"), P("probe", None))
    return jax.shard_map(
        body,
        mesh=mesh,
        in_specs=placed,
        out_specs=(P("probe", "snp"), P(None, "probe"), P()),
        check_vma=False,
    )
```

```python
import functools

import jax
import jax.numpy as jnp
from jax import lax
from jax.experimental import pallas as pl
from jax.experimental.pallas import tpu as pltpu
from jax.sharding import PartitionSpec as P

BOTH = ("snp", "probe")
ACROSS = (((1,), (1,)), ((), ()))
CHUNKS = 4


def first_kernel(
    dosage, freq_hbm, probes_hbm, send, stage, freq, probes, sems, *, snp_count, probe_count, columns
):
    samples, width = dosage.shape
    rows = probes.shape[0]
    part = samples // (snp_count * probe_count)
    step = width // CHUNKS
    copies = [
        pltpu.make_async_copy(dosage.at[:, pl.ds(c * step, step)], stage.at[c], sems.at[c])
        for c in range(CHUNKS)
    ]
    small = [
        pltpu.make_async_copy(freq_hbm, freq, sems.at[CHUNKS]),
        pltpu.make_async_copy(probes_hbm, probes, sems.at[CHUNKS + 1]),
    ]
    for copy in small + copies:
        copy.start()
    group = lax.axis_index("probe")
    row = lax.broadcasted_iota(jnp.int32, (snp_count * part, samples), 0)
    col = lax.broadcasted_iota(jnp.int32, (snp_count * part, samples), 1)
    owner = row // part
    wanted = owner * (part * probe_count) + group * part + (row - owner * part)
    pick = jnp.where(col == wanted, 1.0, 0.0).astype(jnp.bfloat16)
    for copy in small:
        copy.wait()
    signs = probes[...]
    left = jnp.concatenate([signs, pick], axis=0)
    total = jnp.zeros((left.shape[0], samples), jnp.float32)
    for c in range(CHUNKS):
        f = freq[:, c * step : (c + 1) * step]
        mean = 2.0 * f
        scaling = lax.rsqrt(mean * (1.0 - f))
        copies[c].wait()
        standard = ((stage[c].astype(jnp.float32) - mean) * scaling).astype(jnp.bfloat16)
        projected = jnp.dot(left, standard, preferred_element_type=jnp.float32)
        total = total + lax.dot_general(
            projected.astype(jnp.bfloat16), standard, ACROSS, preferred_element_type=jnp.float32
        )
    total = total * (1.0 / columns)
    signed = (signs.astype(jnp.float32) * total[:rows]).astype(jnp.bfloat16)
    kinship = total[rows:].astype(jnp.bfloat16)
    for i in range(snp_count):
        block = jnp.concatenate([signed, kinship[i * part : (i + 1) * part]], axis=0)
        for q in range(probe_count):
            send[i * probe_count + q] = block


def second_kernel(got, probes, kin_twice, forms, estimates, sums, *, snp_count, probe_count):
    rows, samples = probes.shape
    part = got.shape[1] - rows
    group = lax.axis_index("probe")
    for q in range(probe_count):
        summed = got[q].astype(jnp.float32)
        for j in range(1, snp_count):
            summed = summed + got[j * probe_count + q].astype(jnp.float32)
        sums[q] = summed
    everyone = sums[:, :rows]
    rounded = everyone.astype(jnp.bfloat16)
    scale = 1.0 / samples
    first_all = jnp.sum(everyone) * scale
    second_all = jnp.sum(rounded.astype(jnp.float32) * everyone) * scale
    mean = 1.0 / (rows * probe_count)
    lane = lax.broadcasted_iota(jnp.int32, (1, 2), 1)
    estimates[...] = jnp.where(lane == 0, first_all, second_all) * mean
    mine = sums[group][:rows]
    mine_round = mine.astype(jnp.bfloat16)
    first = jnp.sum(mine, axis=1, keepdims=True) * scale
    second = jnp.sum(mine_round.astype(jnp.float32) * mine, axis=1, keepdims=True) * scale
    at = lax.broadcasted_iota(jnp.int32, (rows, rows), 0)
    on = at == lax.broadcasted_iota(jnp.int32, (rows, rows), 1)
    forms[0:1] = jnp.sum(jnp.where(on, first, 0.0), axis=0, keepdims=True)
    forms[1:2] = jnp.sum(jnp.where(on, second, 0.0), axis=0, keepdims=True)
    kinship = sums[:, rows:].reshape(probe_count * part, samples)
    high = kinship.astype(jnp.bfloat16)
    low = (kinship - high.astype(jnp.float32)).astype(jnp.bfloat16)
    vectors = probes[...] * mine_round
    kin_twice[...] = lax.dot_general(
        vectors, high, ACROSS, preferred_element_type=jnp.float32
    ) + lax.dot_general(vectors, low, ACROSS, preferred_element_type=jnp.float32)


def body(dosage, allele_freq, probes):
    snp_count = lax.axis_size("snp")
    probe_count = lax.axis_size("probe")
    samples, width = dosage.shape
    rows = probes.shape[0]
    devices = snp_count * probe_count
    part = samples // devices
    vmem = pl.BlockSpec(memory_space=pltpu.VMEM)
    hbm = pl.BlockSpec(memory_space=pltpu.HBM)
    stay = functools.partial(pltpu.with_memory_space_constraint, memory_space=pltpu.HBM)
    params = pltpu.CompilerParams(vmem_limit_bytes=min(56 << 20, max(16 << 20, 16 * samples * width)))
    send = pl.pallas_call(
        functools.partial(
            first_kernel, snp_count=snp_count, probe_count=probe_count, columns=width * snp_count
        ),
        in_specs=[hbm, hbm, hbm],
        out_specs=vmem,
        out_shape=jax.ShapeDtypeStruct((devices, rows + part, samples), jnp.bfloat16),
        scratch_shapes=[
            pltpu.VMEM((CHUNKS, samples, width // CHUNKS), jnp.bfloat16),
            pltpu.VMEM((1, width), jnp.float32),
            pltpu.VMEM((rows, samples), jnp.bfloat16),
            pltpu.SemaphoreType.DMA((CHUNKS + 2,)),
        ],
        compiler_params=params,
        name="first",
    )(*(stay(x) for x in (dosage, allele_freq.reshape(1, width), probes)))
    got = lax.all_to_all(send, BOTH, 0, 0, tiled=True)
    kin_twice, forms, estimates = pl.pallas_call(
        functools.partial(second_kernel, snp_count=snp_count, probe_count=probe_count),
        in_specs=[vmem, vmem],
        out_specs=[vmem, vmem, vmem],
        out_shape=[
            jax.ShapeDtypeStruct((rows, samples // snp_count), jnp.float32),
            jax.ShapeDtypeStruct((2, rows), jnp.float32),
            jax.ShapeDtypeStruct((1, 2), jnp.float32),
        ],
        scratch_shapes=[pltpu.VMEM((probe_count, rows + part, samples), jnp.float32)],
        compiler_params=params,
        name="second",
    )(got, probes)
    return (kin_twice, forms, estimates.reshape(2))


def solution(mesh):
    placed = (P(None, "snp"), P("snp"), P("probe", None))
    return jax.shard_map(
        body,
        mesh=mesh,
        in_specs=placed,
        out_specs=(P("probe", "snp"), P(None, "probe"), P()),
        check_vma=False,
    )
```

```python
import functools

import jax
import jax.numpy as jnp
from jax import lax
from jax.experimental import pallas as pl
from jax.experimental.pallas import tpu as pltpu
from jax.sharding import PartitionSpec as P

BOTH = ("snp", "probe")
ACROSS = (((1,), (1,)), ((), ()))
CHUNKS = 4


def first_kernel(
    dosage, freq_hbm, probes_hbm, send, stage, freq, probes, sems, *, snp_count, probe_count, columns
):
    samples, width = dosage.shape
    rows = probes.shape[0]
    part = samples // (snp_count * probe_count)
    step = width // CHUNKS
    copies = [
        pltpu.make_async_copy(dosage.at[:, pl.ds(c * step, step)], stage.at[c], sems.at[c])
        for c in range(CHUNKS)
    ]
    small = [
        pltpu.make_async_copy(freq_hbm, freq, sems.at[CHUNKS]),
        pltpu.make_async_copy(probes_hbm, probes, sems.at[CHUNKS + 1]),
    ]
    for copy in small + copies:
        copy.start()
    group = lax.axis_index("probe")
    row = lax.broadcasted_iota(jnp.int32, (snp_count * part, samples), 0)
    col = lax.broadcasted_iota(jnp.int32, (snp_count * part, samples), 1)
    owner = row // part
    wanted = owner * (part * probe_count) + group * part + (row - owner * part)
    pick = jnp.where(col == wanted, 1.0, 0.0).astype(jnp.bfloat16)
    for copy in small:
        copy.wait()
    signs = probes[...]
    left = jnp.concatenate([signs, pick], axis=0)
    total = jnp.zeros((left.shape[0], samples), jnp.float32)
    for c in range(CHUNKS):
        f = freq[:, c * step : (c + 1) * step]
        mean = 2.0 * f
        scaling = lax.rsqrt(mean * (1.0 - f))
        copies[c].wait()
        standard = ((stage[c].astype(jnp.float32) - mean) * scaling).astype(jnp.bfloat16)
        projected = jnp.dot(left, standard, preferred_element_type=jnp.float32)
        total = total + lax.dot_general(
            projected.astype(jnp.bfloat16), standard, ACROSS, preferred_element_type=jnp.float32
        )
    total = total * (1.0 / columns)
    signed = (signs.astype(jnp.float32) * total[:rows]).astype(jnp.bfloat16)
    kinship = total[rows:].astype(jnp.bfloat16)
    half = samples // 2
    for i in range(snp_count):
        block = jnp.concatenate([signed, kinship[i * part : (i + 1) * part]], axis=0)
        for q in range(probe_count):
            send[i * probe_count + q] = block[:, (q % 2) * half : (q % 2 + 1) * half]


def sum_kernel(got, share, own, sums, *, snp_count, probe_count, rows):
    part = got.shape[1] - rows
    owned = part * probe_count
    group = lax.axis_index("probe")
    partner = group + 1 - 2 * (group % 2)
    first = jnp.zeros((rows, got.shape[2]), jnp.float32)
    second = first
    for q in range(probe_count):
        summed = got[q].astype(jnp.float32)
        for j in range(1, snp_count):
            summed = summed + got[j * probe_count + q].astype(jnp.float32)
        signed = summed[:rows]
        sums[q] = signed
        share[q * part : (q + 1) * part] = summed[rows:]
        first = first + signed
        second = second + signed.astype(jnp.bfloat16).astype(jnp.float32) * signed
    share[owned : owned + rows] = first
    share[owned + rows : owned + 2 * rows] = second
    share[owned + 2 * rows :] = sums[partner]
    own[...] = sums[group]


def last_kernel(share, other, own, probes, kin_twice, forms, estimates, *, probe_count):
    rows, samples = probes.shape
    half = samples // 2
    owned = share.shape[0] - 3 * rows
    low_half = lax.axis_index("probe") % 2 == 0
    scale = 1.0 / samples
    mean = scale / (rows * probe_count)
    ends = share[owned : owned + 2 * rows] + other[owned : owned + 2 * rows]
    lane = lax.broadcasted_iota(jnp.int32, (1, 2), 1)
    estimates[...] = jnp.where(lane == 0, jnp.sum(ends[:rows]), jnp.sum(ends[rows:])) * mean
    signs = probes[...].astype(jnp.float32)
    signs_low = signs[:, :half]
    signs_high = signs[:, half:]
    first = jnp.zeros((rows, half), jnp.float32)
    second = first
    twice = jnp.zeros((rows, owned), jnp.float32)
    for signed, rest, sign in (
        (own[...], share, jnp.where(low_half, signs_low, signs_high)),
        (other[owned + 2 * rows :], other, jnp.where(low_half, signs_high, signs_low)),
    ):
        rounded = signed.astype(jnp.bfloat16).astype(jnp.float32)
        first = first + signed
        second = second + rounded * signed
        vectors = (sign * rounded).astype(jnp.bfloat16)
        kinship = rest[:owned]
        high = kinship.astype(jnp.bfloat16)
        low = (kinship - high.astype(jnp.float32)).astype(jnp.bfloat16)
        for piece in (high, low):
            twice = twice + lax.dot_general(
                vectors, piece, ACROSS, preferred_element_type=jnp.float32
            )
    kin_twice[...] = twice
    at = lax.broadcasted_iota(jnp.int32, (rows, rows), 0)
    on = at == lax.broadcasted_iota(jnp.int32, (rows, rows), 1)
    for k, form in enumerate((first, second)):
        total = jnp.sum(form, axis=1, keepdims=True) * scale
        forms[k : k + 1] = jnp.sum(jnp.where(on, total, 0.0), axis=0, keepdims=True)


def body(dosage, allele_freq, probes):
    snp_count = lax.axis_size("snp")
    probe_count = lax.axis_size("probe")
    samples, width = dosage.shape
    rows = probes.shape[0]
    devices = snp_count * probe_count
    part = samples // devices
    half = samples // 2
    owned = samples // snp_count
    vmem = pl.BlockSpec(memory_space=pltpu.VMEM)
    hbm = pl.BlockSpec(memory_space=pltpu.HBM)
    stay = functools.partial(pltpu.with_memory_space_constraint, memory_space=pltpu.HBM)
    params = pltpu.CompilerParams(vmem_limit_bytes=min(56 << 20, max(16 << 20, 16 * samples * width)))
    send = pl.pallas_call(
        functools.partial(
            first_kernel, snp_count=snp_count, probe_count=probe_count, columns=width * snp_count
        ),
        in_specs=[hbm, hbm, hbm],
        out_specs=vmem,
        out_shape=jax.ShapeDtypeStruct((devices, rows + part, half), jnp.bfloat16),
        scratch_shapes=[
            pltpu.VMEM((CHUNKS, samples, width // CHUNKS), jnp.bfloat16),
            pltpu.VMEM((1, width), jnp.float32),
            pltpu.VMEM((rows, samples), jnp.bfloat16),
            pltpu.SemaphoreType.DMA((CHUNKS + 2,)),
        ],
        compiler_params=params,
        name="first",
    )(*(stay(x) for x in (dosage, allele_freq.reshape(1, width), probes)))
    got = lax.all_to_all(send, BOTH, 0, 0, tiled=True)
    share, own = pl.pallas_call(
        functools.partial(sum_kernel, snp_count=snp_count, probe_count=probe_count, rows=rows),
        in_specs=[vmem],
        out_specs=[vmem, vmem],
        out_shape=[
            jax.ShapeDtypeStruct((owned + 3 * rows, half), jnp.float32),
            jax.ShapeDtypeStruct((rows, half), jnp.float32),
        ],
        scratch_shapes=[pltpu.VMEM((probe_count, rows, half), jnp.float32)],
        compiler_params=params,
        name="sums",
    )(got)
    other = lax.ppermute(share, "probe", [(q, q ^ 1) for q in range(probe_count)])
    kin_twice, forms, estimates = pl.pallas_call(
        functools.partial(last_kernel, probe_count=probe_count),
        in_specs=[vmem, vmem, vmem, vmem],
        out_specs=[vmem, vmem, vmem],
        out_shape=[
            jax.ShapeDtypeStruct((rows, owned), jnp.float32),
            jax.ShapeDtypeStruct((2, rows), jnp.float32),
            jax.ShapeDtypeStruct((1, 2), jnp.float32),
        ],
        compiler_params=params,
        name="last",
    )(share, other, own, probes)
    return (kin_twice, forms, estimates.reshape(2))


def solution(mesh):
    placed = (P(None, "snp"), P("snp"), P("probe", None))
    return jax.shard_map(
        body,
        mesh=mesh,
        in_specs=placed,
        out_specs=(P("probe", "snp"), P(None, "probe"), P()),
        check_vma=False,
    )
```

```python
import functools

import jax
import jax.numpy as jnp
from jax import lax
from jax.experimental import pallas as pl
from jax.experimental.pallas import tpu as pltpu
from jax.sharding import PartitionSpec as P

BOTH = ("snp", "probe")
ACROSS = (((1,), (1,)), ((), ()))
CHUNKS = 2


def first_kernel(
    dosage, freq_hbm, probes_hbm, send, stage, freq, probes, sems, *, snp_count, probe_count, columns
):
    samples, width = dosage.shape
    rows = probes.shape[0]
    part = samples // (snp_count * probe_count)
    step = width // CHUNKS
    copies = [
        pltpu.make_async_copy(dosage.at[:, pl.ds(c * step, step)], stage.at[c], sems.at[c])
        for c in range(CHUNKS)
    ]
    small = [
        pltpu.make_async_copy(freq_hbm, freq, sems.at[CHUNKS]),
        pltpu.make_async_copy(probes_hbm, probes, sems.at[CHUNKS + 1]),
    ]
    for copy in small + copies:
        copy.start()
    group = lax.axis_index("probe")
    row = lax.broadcasted_iota(jnp.int32, (snp_count * part, samples), 0)
    col = lax.broadcasted_iota(jnp.int32, (snp_count * part, samples), 1)
    owner = row // part
    wanted = owner * (part * probe_count) + group * part + (row - owner * part)
    pick = jnp.where(col == wanted, 1.0, 0.0).astype(jnp.bfloat16)
    for copy in small:
        copy.wait()
    signs = probes[...]
    left = jnp.concatenate([signs, pick], axis=0)
    weight = jnp.sum(left.astype(jnp.float32), axis=1, keepdims=True)
    mean = 2.0 * freq[...]
    square = 1.0 / (mean * (1.0 - 0.5 * mean))
    total = jnp.zeros((left.shape[0], samples), jnp.float32)
    shift = jnp.zeros((left.shape[0], step), jnp.float32)
    for c in range(CHUNKS):
        m = mean[:, c * step : (c + 1) * step]
        copies[c].wait()
        raw = jnp.dot(left, stage[c], preferred_element_type=jnp.float32)
        if c:
            total = total + lax.dot_general(
                scaled, stage[c - 1], ACROSS, preferred_element_type=jnp.float32
            )
        scaled = ((raw - weight * m) * square[:, c * step : (c + 1) * step]).astype(jnp.bfloat16)
        shift = shift + scaled.astype(jnp.float32) * m
    total = total + lax.dot_general(
        scaled, stage[CHUNKS - 1], ACROSS, preferred_element_type=jnp.float32
    )
    total = (total - jnp.sum(shift, axis=1, keepdims=True)) * (1.0 / columns)
    signed = (signs.astype(jnp.float32) * total[:rows]).astype(jnp.bfloat16)
    kinship = total[rows:].astype(jnp.bfloat16)
    half = samples // 2
    for i in range(snp_count):
        block = jnp.concatenate([signed, kinship[i * part : (i + 1) * part]], axis=0)
        for q in range(probe_count):
            send[i * probe_count + q] = block[:, (q % 2) * half : (q % 2 + 1) * half]


def sum_kernel(got, share, own, sums, *, snp_count, probe_count, rows):
    part = got.shape[1] - rows
    owned = part * probe_count
    group = lax.axis_index("probe")
    partner = group + 1 - 2 * (group % 2)
    first = jnp.zeros((rows, got.shape[2]), jnp.float32)
    second = first
    for q in range(probe_count):
        summed = got[q].astype(jnp.float32)
        for j in range(1, snp_count):
            summed = summed + got[j * probe_count + q].astype(jnp.float32)
        signed = summed[:rows]
        sums[q] = signed
        share[q * part : (q + 1) * part] = summed[rows:]
        first = first + signed
        second = second + signed.astype(jnp.bfloat16).astype(jnp.float32) * signed
    share[owned : owned + rows] = first
    share[owned + rows : owned + 2 * rows] = second
    share[owned + 2 * rows :] = sums[partner]
    own[...] = sums[group]


def last_kernel(share, other, own, probes, kin_twice, forms, estimates, *, probe_count):
    rows, samples = probes.shape
    half = samples // 2
    owned = share.shape[0] - 3 * rows
    low_half = lax.axis_index("probe") % 2 == 0
    scale = 1.0 / samples
    mean = scale / (rows * probe_count)
    ends = share[owned : owned + 2 * rows] + other[owned : owned + 2 * rows]
    lane = lax.broadcasted_iota(jnp.int32, (1, 2), 1)
    estimates[...] = jnp.where(lane == 0, jnp.sum(ends[:rows]), jnp.sum(ends[rows:])) * mean
    signs = probes[...].astype(jnp.float32)
    signs_low = signs[:, :half]
    signs_high = signs[:, half:]
    first = jnp.zeros((rows, half), jnp.float32)
    second = first
    twice = jnp.zeros((rows, owned), jnp.float32)
    for signed, rest, sign in (
        (own[...], share, jnp.where(low_half, signs_low, signs_high)),
        (other[owned + 2 * rows :], other, jnp.where(low_half, signs_high, signs_low)),
    ):
        rounded = signed.astype(jnp.bfloat16).astype(jnp.float32)
        first = first + signed
        second = second + rounded * signed
        vectors = (sign * rounded).astype(jnp.bfloat16)
        kinship = rest[:owned]
        high = kinship.astype(jnp.bfloat16)
        low = (kinship - high.astype(jnp.float32)).astype(jnp.bfloat16)
        for piece in (high, low):
            twice = twice + lax.dot_general(
                vectors, piece, ACROSS, preferred_element_type=jnp.float32
            )
    kin_twice[...] = twice
    at = lax.broadcasted_iota(jnp.int32, (rows, rows), 0)
    on = at == lax.broadcasted_iota(jnp.int32, (rows, rows), 1)
    for k, form in enumerate((first, second)):
        total = jnp.sum(form, axis=1, keepdims=True) * scale
        forms[k : k + 1] = jnp.sum(jnp.where(on, total, 0.0), axis=0, keepdims=True)


def body(dosage, allele_freq, probes):
    snp_count = lax.axis_size("snp")
    probe_count = lax.axis_size("probe")
    samples, width = dosage.shape
    rows = probes.shape[0]
    devices = snp_count * probe_count
    part = samples // devices
    half = samples // 2
    owned = samples // snp_count
    vmem = pl.BlockSpec(memory_space=pltpu.VMEM)
    hbm = pl.BlockSpec(memory_space=pltpu.HBM)
    stay = functools.partial(pltpu.with_memory_space_constraint, memory_space=pltpu.HBM)
    params = pltpu.CompilerParams(vmem_limit_bytes=min(56 << 20, max(16 << 20, 16 * samples * width)))
    send = pl.pallas_call(
        functools.partial(
            first_kernel, snp_count=snp_count, probe_count=probe_count, columns=width * snp_count
        ),
        in_specs=[hbm, hbm, hbm],
        out_specs=vmem,
        out_shape=jax.ShapeDtypeStruct((devices, rows + part, half), jnp.bfloat16),
        scratch_shapes=[
            pltpu.VMEM((CHUNKS, samples, width // CHUNKS), jnp.bfloat16),
            pltpu.VMEM((1, width), jnp.float32),
            pltpu.VMEM((rows, samples), jnp.bfloat16),
            pltpu.SemaphoreType.DMA((CHUNKS + 2,)),
        ],
        compiler_params=params,
        name="first",
    )(*(stay(x) for x in (dosage, allele_freq.reshape(1, width), probes)))
    got = lax.all_to_all(send, BOTH, 0, 0, tiled=True)
    share, own = pl.pallas_call(
        functools.partial(sum_kernel, snp_count=snp_count, probe_count=probe_count, rows=rows),
        in_specs=[vmem],
        out_specs=[vmem, vmem],
        out_shape=[
            jax.ShapeDtypeStruct((owned + 3 * rows, half), jnp.float32),
            jax.ShapeDtypeStruct((rows, half), jnp.float32),
        ],
        scratch_shapes=[pltpu.VMEM((probe_count, rows, half), jnp.float32)],
        compiler_params=params,
        name="sums",
    )(got)
    other = lax.ppermute(share, "probe", [(q, q ^ 1) for q in range(probe_count)])
    kin_twice, forms, estimates = pl.pallas_call(
        functools.partial(last_kernel, probe_count=probe_count),
        in_specs=[vmem, vmem, vmem, vmem],
        out_specs=[vmem, vmem, vmem],
        out_shape=[
            jax.ShapeDtypeStruct((rows, owned), jnp.float32),
            jax.ShapeDtypeStruct((2, rows), jnp.float32),
            jax.ShapeDtypeStruct((1, 2), jnp.float32),
        ],
        compiler_params=params,
        name="last",
    )(share, other, own, probes)
    return (kin_twice, forms, estimates.reshape(2))


def solution(mesh):
    placed = (P(None, "snp"), P("snp"), P("probe", None))
    return jax.shard_map(
        body,
        mesh=mesh,
        in_specs=placed,
        out_specs=(P("probe", "snp"), P(None, "probe"), P()),
        check_vma=False,
    )
```

```python
import functools

import jax
import jax.numpy as jnp
from jax import lax
from jax.experimental import pallas as pl
from jax.experimental.pallas import tpu as pltpu
from jax.sharding import PartitionSpec as P

BOTH = ("probe", "snp")
ACROSS = (((1,), (1,)), ((), ()))
CHUNKS = 2


def first_kernel(
    dosage, freq_hbm, probes_hbm, send, stage, freq, probes, sems, *, snp_count, probe_count, columns
):
    samples, width = dosage.shape
    rows = probes.shape[0]
    part = samples // (snp_count * probe_count)
    step = width // CHUNKS
    copies = [
        pltpu.make_async_copy(dosage.at[:, pl.ds(c * step, step)], stage.at[c], sems.at[c])
        for c in range(CHUNKS)
    ]
    small = [
        pltpu.make_async_copy(freq_hbm, freq, sems.at[CHUNKS]),
        pltpu.make_async_copy(probes_hbm, probes, sems.at[CHUNKS + 1]),
    ]
    for copy in small + copies:
        copy.start()
    group = lax.axis_index("probe")
    row = lax.broadcasted_iota(jnp.int32, (snp_count * part, samples), 0)
    col = lax.broadcasted_iota(jnp.int32, (snp_count * part, samples), 1)
    owner = row // part
    wanted = owner * (part * probe_count) + group * part + (row - owner * part)
    pick = jnp.where(col == wanted, 1.0, 0.0).astype(jnp.bfloat16)
    for copy in small:
        copy.wait()
    signs = probes[...]
    left = jnp.concatenate([signs, pick], axis=0)
    weight = jnp.sum(left.astype(jnp.float32), axis=1, keepdims=True)
    mean = 2.0 * freq[...]
    square = 1.0 / (mean * (1.0 - 0.5 * mean))
    total = jnp.zeros((left.shape[0], samples), jnp.float32)
    shift = jnp.zeros((left.shape[0], step), jnp.float32)
    for c in range(CHUNKS):
        m = mean[:, c * step : (c + 1) * step]
        copies[c].wait()
        raw = jnp.dot(left, stage[c], preferred_element_type=jnp.float32)
        if c:
            total = total + lax.dot_general(
                scaled, stage[c - 1], ACROSS, preferred_element_type=jnp.float32
            )
        scaled = ((raw - weight * m) * square[:, c * step : (c + 1) * step]).astype(jnp.bfloat16)
        shift = shift + scaled.astype(jnp.float32) * m
    total = total + lax.dot_general(
        scaled, stage[CHUNKS - 1], ACROSS, preferred_element_type=jnp.float32
    )
    total = (total - jnp.sum(shift, axis=1, keepdims=True)) * (1.0 / columns)
    signed = (signs.astype(jnp.float32) * total[:rows]).astype(jnp.bfloat16)
    kinship = total[rows:].astype(jnp.bfloat16)
    half = samples // 2
    for i in range(snp_count):
        block = jnp.concatenate([signed, kinship[i * part : (i + 1) * part]], axis=0)
        for q in range(probe_count):
            send[q * snp_count + i] = block[:, (q % 2) * half : (q % 2 + 1) * half]


def sum_kernel(got, share, own, sums, *, snp_count, probe_count, rows):
    part = got.shape[1] - rows
    owned = part * probe_count
    group = lax.axis_index("probe")
    partner = group + 1 - 2 * (group % 2)
    first = jnp.zeros((rows, got.shape[2]), jnp.float32)
    second = first
    for q in range(probe_count):
        summed = got[q * snp_count].astype(jnp.float32)
        for j in range(1, snp_count):
            summed = summed + got[q * snp_count + j].astype(jnp.float32)
        signed = summed[:rows]
        sums[q] = signed
        share[q * part : (q + 1) * part] = summed[rows:]
        first = first + signed
        second = second + signed.astype(jnp.bfloat16).astype(jnp.float32) * signed
    share[owned : owned + rows] = first
    share[owned + rows : owned + 2 * rows] = second
    share[owned + 2 * rows :] = sums[partner]
    own[...] = sums[group]


def last_kernel(share, other, own, probes, kin_twice, forms, estimates, *, probe_count):
    rows, samples = probes.shape
    half = samples // 2
    owned = share.shape[0] - 3 * rows
    low_half = lax.axis_index("probe") % 2 == 0
    scale = 1.0 / samples
    mean = scale / (rows * probe_count)
    ends = share[owned : owned + 2 * rows] + other[owned : owned + 2 * rows]
    lane = lax.broadcasted_iota(jnp.int32, (1, 2), 1)
    estimates[...] = jnp.where(lane == 0, jnp.sum(ends[:rows]), jnp.sum(ends[rows:])) * mean
    signs = probes[...].astype(jnp.float32)
    signs_low = signs[:, :half]
    signs_high = signs[:, half:]
    first = jnp.zeros((rows, half), jnp.float32)
    second = first
    twice = jnp.zeros((rows, owned), jnp.float32)
    for signed, rest, sign in (
        (own[...], share, jnp.where(low_half, signs_low, signs_high)),
        (other[owned + 2 * rows :], other, jnp.where(low_half, signs_high, signs_low)),
    ):
        rounded = signed.astype(jnp.bfloat16).astype(jnp.float32)
        first = first + signed
        second = second + rounded * signed
        vectors = (sign * rounded).astype(jnp.bfloat16)
        kinship = rest[:owned]
        high = kinship.astype(jnp.bfloat16)
        low = (kinship - high.astype(jnp.float32)).astype(jnp.bfloat16)
        for piece in (high, low):
            twice = twice + lax.dot_general(
                vectors, piece, ACROSS, preferred_element_type=jnp.float32
            )
    kin_twice[...] = twice
    at = lax.broadcasted_iota(jnp.int32, (rows, rows), 0)
    on = at == lax.broadcasted_iota(jnp.int32, (rows, rows), 1)
    for k, form in enumerate((first, second)):
        total = jnp.sum(form, axis=1, keepdims=True) * scale
        forms[k : k + 1] = jnp.sum(jnp.where(on, total, 0.0), axis=0, keepdims=True)


def body(dosage, allele_freq, probes):
    snp_count = lax.axis_size("snp")
    probe_count = lax.axis_size("probe")
    samples, width = dosage.shape
    rows = probes.shape[0]
    devices = snp_count * probe_count
    part = samples // devices
    half = samples // 2
    owned = samples // snp_count
    vmem = pl.BlockSpec(memory_space=pltpu.VMEM)
    hbm = pl.BlockSpec(memory_space=pltpu.HBM)
    stay = functools.partial(pltpu.with_memory_space_constraint, memory_space=pltpu.HBM)
    params = pltpu.CompilerParams(vmem_limit_bytes=min(56 << 20, max(16 << 20, 16 * samples * width)))
    send = pl.pallas_call(
        functools.partial(
            first_kernel, snp_count=snp_count, probe_count=probe_count, columns=width * snp_count
        ),
        in_specs=[hbm, hbm, hbm],
        out_specs=vmem,
        out_shape=jax.ShapeDtypeStruct((devices, rows + part, half), jnp.bfloat16),
        scratch_shapes=[
            pltpu.VMEM((CHUNKS, samples, width // CHUNKS), jnp.bfloat16),
            pltpu.VMEM((1, width), jnp.float32),
            pltpu.VMEM((rows, samples), jnp.bfloat16),
            pltpu.SemaphoreType.DMA((CHUNKS + 2,)),
        ],
        compiler_params=params,
        name="first",
    )(*(stay(x) for x in (dosage, allele_freq.reshape(1, width), probes)))
    got = lax.all_to_all(send, BOTH, 0, 0, tiled=True)
    share, own = pl.pallas_call(
        functools.partial(sum_kernel, snp_count=snp_count, probe_count=probe_count, rows=rows),
        in_specs=[vmem],
        out_specs=[vmem, vmem],
        out_shape=[
            jax.ShapeDtypeStruct((owned + 3 * rows, half), jnp.float32),
            jax.ShapeDtypeStruct((rows, half), jnp.float32),
        ],
        scratch_shapes=[pltpu.VMEM((probe_count, rows, half), jnp.float32)],
        compiler_params=params,
        name="sums",
    )(got)
    other = lax.ppermute(share, "probe", [(q, q ^ 1) for q in range(probe_count)])
    kin_twice, forms, estimates = pl.pallas_call(
        functools.partial(last_kernel, probe_count=probe_count),
        in_specs=[vmem, vmem, vmem, vmem],
        out_specs=[vmem, vmem, vmem],
        out_shape=[
            jax.ShapeDtypeStruct((rows, owned), jnp.float32),
            jax.ShapeDtypeStruct((2, rows), jnp.float32),
            jax.ShapeDtypeStruct((1, 2), jnp.float32),
        ],
        compiler_params=params,
        name="last",
    )(share, other, own, probes)
    return (kin_twice, forms, estimates.reshape(2))


def solution(mesh):
    placed = (P(None, "snp"), P("snp"), P("probe", None))
    return jax.shard_map(
        body,
        mesh=mesh,
        in_specs=placed,
        out_specs=(P("probe", "snp"), P(None, "probe"), P()),
        check_vma=False,
    )
```

```python
import functools

import jax
import jax.numpy as jnp
from jax import lax
from jax.experimental import pallas as pl
from jax.experimental.pallas import tpu as pltpu
from jax.sharding import PartitionSpec as P

BOTH = ("probe", "snp")
ACROSS = (((1,), (1,)), ((), ()))
CHUNKS = 2
TILE = 256


def tiled_products(left, weight, mean, square, copies, stage):
    height = left.shape[0]
    acc = [pltpu.ACC(q)((height, TILE), jnp.float32) for q in (0, 1) for _ in range(3)]
    width = stage.shape[2]

    def run(raw00, raw01, sum0, raw10, raw11, sum1):
        raws = ((raw00, raw01), (raw10, raw11))
        sums = (sum0, sum1)
        shift = jnp.zeros((height, TILE), jnp.float32)
        for c, copy in enumerate(copies):
            copy.wait()

            def tile(k, q):
                return slice((2 * k + q) * TILE, (2 * k + q + 1) * TILE)

            for k in (0, 1):
                for q in (0, 1):
                    pltpu.matmul_push_rhs(stage[c, :, tile(k, q)], k, q)
            for k in (0, 1):
                for q in (0, 1):
                    pltpu.matmul_acc_lhs(raws[q][k], left, load_staged_rhs=k)
                    pltpu.matmul_push_rhs(stage[c, :, tile(k, q)], k, q, transpose=True)
            for k in (0, 1):
                for q in (0, 1):
                    at = slice(c * width + tile(k, q).start, c * width + tile(k, q).stop)
                    m = mean[:, at]
                    raw = pltpu.matmul_pop(raws[q][k])
                    scaled = ((raw - weight * m) * square[:, at]).astype(jnp.bfloat16)
                    pltpu.matmul_acc_lhs(sums[q], scaled, load_staged_rhs=k)
                    shift = shift + scaled.astype(jnp.float32) * m
        return pltpu.matmul_pop(sum0) + pltpu.matmul_pop(sum1), shift

    return pl.run_scoped(run, *acc)


def first_kernel(
    dosage, freq_hbm, probes_hbm, send, stage, freq, probes, sems, *, snp_count, probe_count, columns
):
    samples, width = dosage.shape
    rows = probes.shape[0]
    part = samples // (snp_count * probe_count)
    step = width // CHUNKS
    copies = [
        pltpu.make_async_copy(dosage.at[:, pl.ds(c * step, step)], stage.at[c], sems.at[c])
        for c in range(CHUNKS)
    ]
    small = [
        pltpu.make_async_copy(freq_hbm, freq, sems.at[CHUNKS]),
        pltpu.make_async_copy(probes_hbm, probes, sems.at[CHUNKS + 1]),
    ]
    for copy in small + copies:
        copy.start()
    group = lax.axis_index("probe")
    row = lax.broadcasted_iota(jnp.int32, (snp_count * part, samples), 0)
    col = lax.broadcasted_iota(jnp.int32, (snp_count * part, samples), 1)
    owner = row // part
    wanted = owner * (part * probe_count) + group * part + (row - owner * part)
    pick = jnp.where(col == wanted, 1.0, 0.0).astype(jnp.bfloat16)
    for copy in small:
        copy.wait()
    signs = probes[...]
    blank = jnp.zeros((-(rows + pick.shape[0]) % 16, samples), jnp.bfloat16)
    left = jnp.concatenate([signs, pick, blank], axis=0)
    weight = jnp.sum(left.astype(jnp.float32), axis=1, keepdims=True)
    mean = 2.0 * freq[...]
    square = 1.0 / (mean * (1.0 - 0.5 * mean))
    if samples == TILE and step == 4 * TILE:
        total, shift = tiled_products(left, weight, mean, square, copies, stage)
    else:
        total = jnp.zeros((left.shape[0], samples), jnp.float32)
        shift = jnp.zeros((left.shape[0], step), jnp.float32)
        for c in range(CHUNKS):
            m = mean[:, c * step : (c + 1) * step]
            copies[c].wait()
            raw = jnp.dot(left, stage[c], preferred_element_type=jnp.float32)
            if c:
                total = total + lax.dot_general(
                    scaled, stage[c - 1], ACROSS, preferred_element_type=jnp.float32
                )
            scaled = raw - weight * m
            scaled = (scaled * square[:, c * step : (c + 1) * step]).astype(jnp.bfloat16)
            shift = shift + scaled.astype(jnp.float32) * m
        total = total + lax.dot_general(
            scaled, stage[CHUNKS - 1], ACROSS, preferred_element_type=jnp.float32
        )
    total = (total - jnp.sum(shift, axis=1, keepdims=True)) * (1.0 / columns)
    signed = (signs.astype(jnp.float32) * total[:rows]).astype(jnp.bfloat16)
    kinship = total[rows:].astype(jnp.bfloat16)
    half = samples // 2
    for i in range(snp_count):
        block = jnp.concatenate([signed, kinship[i * part : (i + 1) * part]], axis=0)
        for q in range(probe_count):
            send[q * snp_count + i] = block[:, (q % 2) * half : (q % 2 + 1) * half]


def sum_kernel(got, share, own, sums, *, snp_count, probe_count, rows):
    part = got.shape[1] - rows
    owned = part * probe_count
    group = lax.axis_index("probe")
    partner = group + 1 - 2 * (group % 2)
    first = jnp.zeros((rows, got.shape[2]), jnp.float32)
    second = first
    for q in range(probe_count):
        summed = got[q * snp_count].astype(jnp.float32)
        for j in range(1, snp_count):
            summed = summed + got[q * snp_count + j].astype(jnp.float32)
        signed = summed[:rows]
        sums[q] = signed
        share[q * part : (q + 1) * part] = summed[rows:]
        first = first + signed
        second = second + signed.astype(jnp.bfloat16).astype(jnp.float32) * signed
    share[owned : owned + rows] = first
    share[owned + rows : owned + 2 * rows] = second
    share[owned + 2 * rows :] = sums[partner]
    own[...] = sums[group]


def last_kernel(share, other, own, probes, kin_twice, forms, estimates, *, probe_count):
    rows, samples = probes.shape
    half = samples // 2
    owned = share.shape[0] - 3 * rows
    low_half = lax.axis_index("probe") % 2 == 0
    scale = 1.0 / samples
    mean = scale / (rows * probe_count)
    ends = share[owned : owned + 2 * rows] + other[owned : owned + 2 * rows]
    lane = lax.broadcasted_iota(jnp.int32, (1, 2), 1)
    estimates[...] = jnp.where(lane == 0, jnp.sum(ends[:rows]), jnp.sum(ends[rows:])) * mean
    signs = probes[...].astype(jnp.float32)
    signs_low = signs[:, :half]
    signs_high = signs[:, half:]
    first = jnp.zeros((rows, half), jnp.float32)
    second = first
    twice = jnp.zeros((rows, owned), jnp.float32)
    for signed, rest, sign in (
        (own[...], share, jnp.where(low_half, signs_low, signs_high)),
        (other[owned + 2 * rows :], other, jnp.where(low_half, signs_high, signs_low)),
    ):
        rounded = signed.astype(jnp.bfloat16).astype(jnp.float32)
        first = first + signed
        second = second + rounded * signed
        vectors = (sign * rounded).astype(jnp.bfloat16)
        kinship = rest[:owned]
        high = kinship.astype(jnp.bfloat16)
        low = (kinship - high.astype(jnp.float32)).astype(jnp.bfloat16)
        for piece in (high, low):
            twice = twice + lax.dot_general(
                vectors, piece, ACROSS, preferred_element_type=jnp.float32
            )
    kin_twice[...] = twice
    at = lax.broadcasted_iota(jnp.int32, (rows, rows), 0)
    on = at == lax.broadcasted_iota(jnp.int32, (rows, rows), 1)
    for k, form in enumerate((first, second)):
        total = jnp.sum(form, axis=1, keepdims=True) * scale
        forms[k : k + 1] = jnp.sum(jnp.where(on, total, 0.0), axis=0, keepdims=True)


def body(dosage, allele_freq, probes):
    snp_count = lax.axis_size("snp")
    probe_count = lax.axis_size("probe")
    samples, width = dosage.shape
    rows = probes.shape[0]
    devices = snp_count * probe_count
    part = samples // devices
    half = samples // 2
    owned = samples // snp_count
    vmem = pl.BlockSpec(memory_space=pltpu.VMEM)
    hbm = pl.BlockSpec(memory_space=pltpu.HBM)
    stay = functools.partial(pltpu.with_memory_space_constraint, memory_space=pltpu.HBM)
    params = pltpu.CompilerParams(vmem_limit_bytes=min(56 << 20, max(16 << 20, 16 * samples * width)))
    send = pl.pallas_call(
        functools.partial(
            first_kernel, snp_count=snp_count, probe_count=probe_count, columns=width * snp_count
        ),
        in_specs=[hbm, hbm, hbm],
        out_specs=vmem,
        out_shape=jax.ShapeDtypeStruct((devices, rows + part, half), jnp.bfloat16),
        scratch_shapes=[
            pltpu.VMEM((CHUNKS, samples, width // CHUNKS), jnp.bfloat16),
            pltpu.VMEM((1, width), jnp.float32),
            pltpu.VMEM((rows, samples), jnp.bfloat16),
            pltpu.SemaphoreType.DMA((CHUNKS + 2,)),
        ],
        compiler_params=params,
        name="first",
    )(*(stay(x) for x in (dosage, allele_freq.reshape(1, width), probes)))
    got = lax.all_to_all(send, BOTH, 0, 0, tiled=True)
    share, own = pl.pallas_call(
        functools.partial(sum_kernel, snp_count=snp_count, probe_count=probe_count, rows=rows),
        in_specs=[vmem],
        out_specs=[vmem, vmem],
        out_shape=[
            jax.ShapeDtypeStruct((owned + 3 * rows, half), jnp.float32),
            jax.ShapeDtypeStruct((rows, half), jnp.float32),
        ],
        scratch_shapes=[pltpu.VMEM((probe_count, rows, half), jnp.float32)],
        compiler_params=params,
        name="sums",
    )(got)
    other = lax.ppermute(share, "probe", [(q, q ^ 1) for q in range(probe_count)])
    kin_twice, forms, estimates = pl.pallas_call(
        functools.partial(last_kernel, probe_count=probe_count),
        in_specs=[vmem, vmem, vmem, vmem],
        out_specs=[vmem, vmem, vmem],
        out_shape=[
            jax.ShapeDtypeStruct((rows, owned), jnp.float32),
            jax.ShapeDtypeStruct((2, rows), jnp.float32),
            jax.ShapeDtypeStruct((1, 2), jnp.float32),
        ],
        compiler_params=params,
        name="last",
    )(share, other, own, probes)
    return (kin_twice, forms, estimates.reshape(2))


def solution(mesh):
    placed = (P(None, "snp"), P("snp"), P("probe", None))
    return jax.shard_map(
        body,
        mesh=mesh,
        in_specs=placed,
        out_specs=(P("probe", "snp"), P(None, "probe"), P()),
        check_vma=False,
    )
```

```python
import functools

import jax
import jax.numpy as jnp
from jax import lax
from jax.experimental import pallas as pl
from jax.experimental.pallas import tpu as pltpu
from jax.sharding import PartitionSpec as P

BOTH = ("probe", "snp")
ACROSS = (((1,), (1,)), ((), ()))
CHUNKS = 2
TILE = 256


def tiled_products(left, weight, mean, square, copies, stage):
    height = left.shape[0]
    acc = [pltpu.ACC(q)((height, TILE), jnp.float32) for q in (0, 1) for _ in range(3)]
    width = stage.shape[2]

    def run(raw00, raw01, sum0, raw10, raw11, sum1):
        raws = ((raw00, raw01), (raw10, raw11))
        sums = (sum0, sum1)
        shift = jnp.zeros((height, TILE), jnp.float32)
        for ref in (*raws[0], *raws[1], *sums):
            pltpu.matmul_pop(ref)
        for c, copy in enumerate(copies):
            copy.wait()

            def tile(k, q):
                return slice((2 * k + q) * TILE, (2 * k + q + 1) * TILE)

            for k in (0, 1):
                for q in (0, 1):
                    pltpu.matmul_push_rhs(stage[c, :, tile(k, q)], k, q)
            for k in (0, 1):
                for q in (0, 1):
                    pltpu.matmul_acc_lhs(raws[q][k], left, load_staged_rhs=k)
                    pltpu.matmul_push_rhs(stage[c, :, tile(k, q)], k, q, transpose=True)
            for k in (0, 1):
                for q in (0, 1):
                    at = slice(c * width + tile(k, q).start, c * width + tile(k, q).stop)
                    m = mean[:, at]
                    raw = pltpu.matmul_pop(raws[q][k])
                    scaled = ((raw - weight * m) * square[:, at]).astype(jnp.bfloat16)
                    pltpu.matmul_acc_lhs(sums[q], scaled, load_staged_rhs=k)
                    shift = shift + scaled.astype(jnp.float32) * m
        return pltpu.matmul_pop(sum0) + pltpu.matmul_pop(sum1), shift

    return pl.run_scoped(run, *acc)


def first_kernel(
    dosage, freq_hbm, probes_hbm, send, stage, freq, probes, sems, *, snp_count, probe_count, columns
):
    samples, width = dosage.shape
    rows = probes.shape[0]
    part = samples // (snp_count * probe_count)
    step = width // CHUNKS
    copies = [
        pltpu.make_async_copy(dosage.at[:, pl.ds(c * step, step)], stage.at[c], sems.at[c])
        for c in range(CHUNKS)
    ]
    small = [
        pltpu.make_async_copy(freq_hbm, freq, sems.at[CHUNKS]),
        pltpu.make_async_copy(probes_hbm, probes, sems.at[CHUNKS + 1]),
    ]
    for copy in small + copies:
        copy.start()
    group = lax.axis_index("probe")
    row = lax.broadcasted_iota(jnp.int32, (snp_count * part, samples), 0)
    col = lax.broadcasted_iota(jnp.int32, (snp_count * part, samples), 1)
    owner = row // part
    wanted = owner * (part * probe_count) + group * part + (row - owner * part)
    pick = jnp.where(col == wanted, 1.0, 0.0).astype(jnp.bfloat16)
    for copy in small:
        copy.wait()
    signs = probes[...]
    blank = jnp.zeros((-(rows + pick.shape[0]) % 16, samples), jnp.bfloat16)
    left = jnp.concatenate([signs, pick, blank], axis=0)
    weight = jnp.sum(left.astype(jnp.float32), axis=1, keepdims=True)
    mean = 2.0 * freq[...]
    square = 1.0 / (mean * (1.0 - 0.5 * mean))
    if samples == TILE and step == 4 * TILE:
        total, shift = tiled_products(left, weight, mean, square, copies, stage)
    else:
        total = jnp.zeros((left.shape[0], samples), jnp.float32)
        shift = jnp.zeros((left.shape[0], step), jnp.float32)
        for c in range(CHUNKS):
            m = mean[:, c * step : (c + 1) * step]
            copies[c].wait()
            raw = jnp.dot(left, stage[c], preferred_element_type=jnp.float32)
            if c:
                total = total + lax.dot_general(
                    scaled, stage[c - 1], ACROSS, preferred_element_type=jnp.float32
                )
            scaled = raw - weight * m
            scaled = (scaled * square[:, c * step : (c + 1) * step]).astype(jnp.bfloat16)
            shift = shift + scaled.astype(jnp.float32) * m
        total = total + lax.dot_general(
            scaled, stage[CHUNKS - 1], ACROSS, preferred_element_type=jnp.float32
        )
    total = (total - jnp.sum(shift, axis=1, keepdims=True)) * (1.0 / columns)
    signed = (signs.astype(jnp.float32) * total[:rows]).astype(jnp.bfloat16)
    kinship = total[rows:].astype(jnp.bfloat16)
    half = samples // 2
    for i in range(snp_count):
        block = jnp.concatenate([signed, kinship[i * part : (i + 1) * part]], axis=0)
        for q in range(probe_count):
            send[q * snp_count + i] = block[:, (q % 2) * half : (q % 2 + 1) * half]


def sum_kernel(got, share, own, sums, *, snp_count, probe_count, rows):
    part = got.shape[1] - rows
    owned = part * probe_count
    group = lax.axis_index("probe")
    partner = group + 1 - 2 * (group % 2)
    first = jnp.zeros((rows, got.shape[2]), jnp.float32)
    second = first
    for q in range(probe_count):
        summed = got[q * snp_count].astype(jnp.float32)
        for j in range(1, snp_count):
            summed = summed + got[q * snp_count + j].astype(jnp.float32)
        signed = summed[:rows]
        sums[q] = signed
        share[q * part : (q + 1) * part] = summed[rows:]
        first = first + signed
        second = second + signed.astype(jnp.bfloat16).astype(jnp.float32) * signed
    share[owned : owned + rows] = first
    share[owned + rows : owned + 2 * rows] = second
    share[owned + 2 * rows :] = sums[partner]
    own[...] = sums[group]


def last_kernel(share, other, own, probes, kin_twice, forms, estimates, *, probe_count):
    rows, samples = probes.shape
    half = samples // 2
    owned = share.shape[0] - 3 * rows
    low_half = lax.axis_index("probe") % 2 == 0
    scale = 1.0 / samples
    mean = scale / (rows * probe_count)
    ends = share[owned : owned + 2 * rows] + other[owned : owned + 2 * rows]
    lane = lax.broadcasted_iota(jnp.int32, (1, 2), 1)
    estimates[...] = jnp.where(lane == 0, jnp.sum(ends[:rows]), jnp.sum(ends[rows:])) * mean
    signs = probes[...].astype(jnp.float32)
    signs_low = signs[:, :half]
    signs_high = signs[:, half:]
    first = jnp.zeros((rows, half), jnp.float32)
    second = first
    twice = jnp.zeros((rows, owned), jnp.float32)
    for signed, rest, sign in (
        (own[...], share, jnp.where(low_half, signs_low, signs_high)),
        (other[owned + 2 * rows :], other, jnp.where(low_half, signs_high, signs_low)),
    ):
        rounded = signed.astype(jnp.bfloat16).astype(jnp.float32)
        first = first + signed
        second = second + rounded * signed
        vectors = (sign * rounded).astype(jnp.bfloat16)
        kinship = rest[:owned]
        high = kinship.astype(jnp.bfloat16)
        low = (kinship - high.astype(jnp.float32)).astype(jnp.bfloat16)
        for piece in (high, low):
            twice = twice + lax.dot_general(
                vectors, piece, ACROSS, preferred_element_type=jnp.float32
            )
    kin_twice[...] = twice
    at = lax.broadcasted_iota(jnp.int32, (rows, rows), 0)
    on = at == lax.broadcasted_iota(jnp.int32, (rows, rows), 1)
    for k, form in enumerate((first, second)):
        total = jnp.sum(form, axis=1, keepdims=True) * scale
        forms[k : k + 1] = jnp.sum(jnp.where(on, total, 0.0), axis=0, keepdims=True)


def body(dosage, allele_freq, probes):
    snp_count = lax.axis_size("snp")
    probe_count = lax.axis_size("probe")
    samples, width = dosage.shape
    rows = probes.shape[0]
    devices = snp_count * probe_count
    part = samples // devices
    half = samples // 2
    owned = samples // snp_count
    vmem = pl.BlockSpec(memory_space=pltpu.VMEM)
    hbm = pl.BlockSpec(memory_space=pltpu.HBM)
    stay = functools.partial(pltpu.with_memory_space_constraint, memory_space=pltpu.HBM)
    params = pltpu.CompilerParams(vmem_limit_bytes=min(56 << 20, max(16 << 20, 16 * samples * width)))
    send = pl.pallas_call(
        functools.partial(
            first_kernel, snp_count=snp_count, probe_count=probe_count, columns=width * snp_count
        ),
        in_specs=[hbm, hbm, hbm],
        out_specs=vmem,
        out_shape=jax.ShapeDtypeStruct((devices, rows + part, half), jnp.bfloat16),
        scratch_shapes=[
            pltpu.VMEM((CHUNKS, samples, width // CHUNKS), jnp.bfloat16),
            pltpu.VMEM((1, width), jnp.float32),
            pltpu.VMEM((rows, samples), jnp.bfloat16),
            pltpu.SemaphoreType.DMA((CHUNKS + 2,)),
        ],
        compiler_params=params,
        name="first",
    )(*(stay(x) for x in (dosage, allele_freq.reshape(1, width), probes)))
    got = lax.all_to_all(send, BOTH, 0, 0, tiled=True)
    share, own = pl.pallas_call(
        functools.partial(sum_kernel, snp_count=snp_count, probe_count=probe_count, rows=rows),
        in_specs=[vmem],
        out_specs=[vmem, vmem],
        out_shape=[
            jax.ShapeDtypeStruct((owned + 3 * rows, half), jnp.float32),
            jax.ShapeDtypeStruct((rows, half), jnp.float32),
        ],
        scratch_shapes=[pltpu.VMEM((probe_count, rows, half), jnp.float32)],
        compiler_params=params,
        name="sums",
    )(got)
    other = lax.ppermute(share, "probe", [(q, q ^ 1) for q in range(probe_count)])
    kin_twice, forms, estimates = pl.pallas_call(
        functools.partial(last_kernel, probe_count=probe_count),
        in_specs=[vmem, vmem, vmem, vmem],
        out_specs=[vmem, vmem, vmem],
        out_shape=[
            jax.ShapeDtypeStruct((rows, owned), jnp.float32),
            jax.ShapeDtypeStruct((2, rows), jnp.float32),
            jax.ShapeDtypeStruct((1, 2), jnp.float32),
        ],
        compiler_params=params,
        name="last",
    )(share, other, own, probes)
    return (kin_twice, forms, estimates.reshape(2))


def solution(mesh):
    placed = (P(None, "snp"), P("snp"), P("probe", None))
    return jax.shard_map(
        body,
        mesh=mesh,
        in_specs=placed,
        out_specs=(P("probe", "snp"), P(None, "probe"), P()),
        check_vma=False,
    )
```

```python
import functools

import jax
import jax.numpy as jnp
from jax import lax
from jax.experimental import pallas as pl
from jax.experimental.pallas import tpu as pltpu
from jax.sharding import PartitionSpec as P

BOTH = ("probe", "snp")
ACROSS = (((1,), (1,)), ((), ()))
CHUNKS = 2
TILE = 256


def tiled_products(left, mean, scaling, copies, stage, standard):
    height = left.shape[0]
    acc = [pltpu.ACC(q)((height, TILE), jnp.float32) for q in (0, 1) for _ in range(3)]
    width = stage.shape[2]

    def run(raw00, raw01, sum0, raw10, raw11, sum1):
        raws = ((raw00, raw01), (raw10, raw11))
        sums = (sum0, sum1)
        for ref in (*raws[0], *raws[1], *sums):
            pltpu.matmul_pop(ref)
        for c, copy in enumerate(copies):
            copy.wait()

            def tile(k, q):
                return slice((2 * k + q) * TILE, (2 * k + q + 1) * TILE)

            for k in (0, 1):
                for q in (0, 1):
                    at = slice(c * width + tile(k, q).start, c * width + tile(k, q).stop)
                    dosages = stage[c, :, tile(k, q)].astype(jnp.float32)
                    standard[c, :, tile(k, q)] = (
                        (dosages - mean[:, at]) * scaling[:, at]
                    ).astype(jnp.bfloat16)
                    pltpu.matmul_push_rhs(standard[c, :, tile(k, q)], k, q)
            for k in (0, 1):
                for q in (0, 1):
                    pltpu.matmul_acc_lhs(raws[q][k], left, load_staged_rhs=k)
                    pltpu.matmul_push_rhs(standard[c, :, tile(k, q)], k, q, transpose=True)
            for k in (0, 1):
                for q in (0, 1):
                    projected = pltpu.matmul_pop(raws[q][k]).astype(jnp.bfloat16)
                    pltpu.matmul_acc_lhs(sums[q], projected, load_staged_rhs=k)
        return pltpu.matmul_pop(sum0) + pltpu.matmul_pop(sum1)

    return pl.run_scoped(run, *acc)


def first_kernel(
    dosage, freq_hbm, probes_hbm, send, stage, standard, freq, probes, sems, *, snp_count, probe_count, columns
):
    samples, width = dosage.shape
    rows = probes.shape[0]
    part = samples // (snp_count * probe_count)
    step = width // CHUNKS
    copies = [
        pltpu.make_async_copy(dosage.at[:, pl.ds(c * step, step)], stage.at[c], sems.at[c])
        for c in range(CHUNKS)
    ]
    small = [
        pltpu.make_async_copy(freq_hbm, freq, sems.at[CHUNKS]),
        pltpu.make_async_copy(probes_hbm, probes, sems.at[CHUNKS + 1]),
    ]
    for copy in small + copies:
        copy.start()
    group = lax.axis_index("probe")
    row = lax.broadcasted_iota(jnp.int32, (snp_count * part, samples), 0)
    col = lax.broadcasted_iota(jnp.int32, (snp_count * part, samples), 1)
    owner = row // part
    wanted = owner * (part * probe_count) + group * part + (row - owner * part)
    pick = jnp.where(col == wanted, 1.0, 0.0).astype(jnp.bfloat16)
    for copy in small:
        copy.wait()
    signs = probes[...]
    blank = jnp.zeros((-(rows + pick.shape[0]) % 16, samples), jnp.bfloat16)
    left = jnp.concatenate([signs, pick, blank], axis=0)
    mean = 2.0 * freq[...]
    scaling = lax.rsqrt(mean * (1.0 - 0.5 * mean))
    if samples == TILE and step == 4 * TILE:
        total = tiled_products(left, mean, scaling, copies, stage, standard)
    else:
        total = jnp.zeros((left.shape[0], samples), jnp.float32)
        for c in range(CHUNKS):
            at = slice(c * step, (c + 1) * step)
            copies[c].wait()
            standard[c] = ((stage[c].astype(jnp.float32) - mean[:, at]) * scaling[:, at]).astype(
                jnp.bfloat16
            )
            projected = jnp.dot(left, standard[c], preferred_element_type=jnp.float32)
            total = total + lax.dot_general(
                projected.astype(jnp.bfloat16),
                standard[c],
                ACROSS,
                preferred_element_type=jnp.float32,
            )
    total = total * (1.0 / columns)
    signed = (signs.astype(jnp.float32) * total[:rows]).astype(jnp.bfloat16)
    kinship = total[rows:].astype(jnp.bfloat16)
    half = samples // 2
    for i in range(snp_count):
        block = jnp.concatenate([signed, kinship[i * part : (i + 1) * part]], axis=0)
        for q in range(probe_count):
            send[q * snp_count + i] = block[:, (q % 2) * half : (q % 2 + 1) * half]


def sum_kernel(got, share, own, sums, *, snp_count, probe_count, rows):
    part = got.shape[1] - rows
    owned = part * probe_count
    group = lax.axis_index("probe")
    partner = group + 1 - 2 * (group % 2)
    first = jnp.zeros((rows, got.shape[2]), jnp.float32)
    second = first
    for q in range(probe_count):
        summed = got[q * snp_count].astype(jnp.float32)
        for j in range(1, snp_count):
            summed = summed + got[q * snp_count + j].astype(jnp.float32)
        signed = summed[:rows]
        sums[q] = signed
        share[q * part : (q + 1) * part] = summed[rows:]
        first = first + signed
        second = second + signed.astype(jnp.bfloat16).astype(jnp.float32) * signed
    share[owned : owned + rows] = first
    share[owned + rows : owned + 2 * rows] = second
    share[owned + 2 * rows :] = sums[partner]
    own[...] = sums[group]


def last_kernel(share, other, own, probes, kin_twice, forms, estimates, *, probe_count):
    rows, samples = probes.shape
    half = samples // 2
    owned = share.shape[0] - 3 * rows
    low_half = lax.axis_index("probe") % 2 == 0
    scale = 1.0 / samples
    mean = scale / (rows * probe_count)
    ends = share[owned : owned + 2 * rows] + other[owned : owned + 2 * rows]
    lane = lax.broadcasted_iota(jnp.int32, (1, 2), 1)
    estimates[...] = jnp.where(lane == 0, jnp.sum(ends[:rows]), jnp.sum(ends[rows:])) * mean
    signs = probes[...].astype(jnp.float32)
    signs_low = signs[:, :half]
    signs_high = signs[:, half:]
    first = jnp.zeros((rows, half), jnp.float32)
    second = first
    twice = jnp.zeros((rows, owned), jnp.float32)
    for signed, rest, sign in (
        (own[...], share, jnp.where(low_half, signs_low, signs_high)),
        (other[owned + 2 * rows :], other, jnp.where(low_half, signs_high, signs_low)),
    ):
        rounded = signed.astype(jnp.bfloat16).astype(jnp.float32)
        first = first + signed
        second = second + rounded * signed
        vectors = (sign * rounded).astype(jnp.bfloat16)
        kinship = rest[:owned]
        high = kinship.astype(jnp.bfloat16)
        low = (kinship - high.astype(jnp.float32)).astype(jnp.bfloat16)
        for piece in (high, low):
            twice = twice + lax.dot_general(
                vectors, piece, ACROSS, preferred_element_type=jnp.float32
            )
    kin_twice[...] = twice
    at = lax.broadcasted_iota(jnp.int32, (rows, rows), 0)
    on = at == lax.broadcasted_iota(jnp.int32, (rows, rows), 1)
    for k, form in enumerate((first, second)):
        total = jnp.sum(form, axis=1, keepdims=True) * scale
        forms[k : k + 1] = jnp.sum(jnp.where(on, total, 0.0), axis=0, keepdims=True)


def body(dosage, allele_freq, probes):
    snp_count = lax.axis_size("snp")
    probe_count = lax.axis_size("probe")
    samples, width = dosage.shape
    rows = probes.shape[0]
    devices = snp_count * probe_count
    part = samples // devices
    half = samples // 2
    owned = samples // snp_count
    vmem = pl.BlockSpec(memory_space=pltpu.VMEM)
    hbm = pl.BlockSpec(memory_space=pltpu.HBM)
    stay = functools.partial(pltpu.with_memory_space_constraint, memory_space=pltpu.HBM)
    params = pltpu.CompilerParams(vmem_limit_bytes=min(56 << 20, max(16 << 20, 16 * samples * width)))
    send = pl.pallas_call(
        functools.partial(
            first_kernel, snp_count=snp_count, probe_count=probe_count, columns=width * snp_count
        ),
        in_specs=[hbm, hbm, hbm],
        out_specs=vmem,
        out_shape=jax.ShapeDtypeStruct((devices, rows + part, half), jnp.bfloat16),
        scratch_shapes=[
            pltpu.VMEM((CHUNKS, samples, width // CHUNKS), jnp.bfloat16),
            pltpu.VMEM((CHUNKS, samples, width // CHUNKS), jnp.bfloat16),
            pltpu.VMEM((1, width), jnp.float32),
            pltpu.VMEM((rows, samples), jnp.bfloat16),
            pltpu.SemaphoreType.DMA((CHUNKS + 2,)),
        ],
        compiler_params=params,
        name="first",
    )(*(stay(x) for x in (dosage, allele_freq.reshape(1, width), probes)))
    got = lax.all_to_all(send, BOTH, 0, 0, tiled=True)
    share, own = pl.pallas_call(
        functools.partial(sum_kernel, snp_count=snp_count, probe_count=probe_count, rows=rows),
        in_specs=[vmem],
        out_specs=[vmem, vmem],
        out_shape=[
            jax.ShapeDtypeStruct((owned + 3 * rows, half), jnp.float32),
            jax.ShapeDtypeStruct((rows, half), jnp.float32),
        ],
        scratch_shapes=[pltpu.VMEM((probe_count, rows, half), jnp.float32)],
        compiler_params=params,
        name="sums",
    )(got)
    other = lax.ppermute(share, "probe", [(q, q ^ 1) for q in range(probe_count)])
    kin_twice, forms, estimates = pl.pallas_call(
        functools.partial(last_kernel, probe_count=probe_count),
        in_specs=[vmem, vmem, vmem, vmem],
        out_specs=[vmem, vmem, vmem],
        out_shape=[
            jax.ShapeDtypeStruct((rows, owned), jnp.float32),
            jax.ShapeDtypeStruct((2, rows), jnp.float32),
            jax.ShapeDtypeStruct((1, 2), jnp.float32),
        ],
        compiler_params=params,
        name="last",
    )(share, other, own, probes)
    return (kin_twice, forms, estimates.reshape(2))


def solution(mesh):
    placed = (P(None, "snp"), P("snp"), P("probe", None))
    return jax.shard_map(
        body,
        mesh=mesh,
        in_specs=placed,
        out_specs=(P("probe", "snp"), P(None, "probe"), P()),
        check_vma=False,
    )
```

```python
import functools

import jax
import jax.numpy as jnp
from jax import lax
from jax.experimental import pallas as pl
from jax.experimental.pallas import tpu as pltpu
from jax.sharding import PartitionSpec as P

BOTH = ("probe", "snp")
ACROSS = (((1,), (1,)), ((), ()))
CHUNKS = 2
TILE = 256


def tiled_products(left, mean, scaling, copies, stage, standard):
    height = left.shape[0]
    acc = [pltpu.ACC(q)((height, TILE), jnp.float32) for q in (0, 1) for _ in range(3)]
    width = stage.shape[2]

    def run(raw00, raw01, sum0, raw10, raw11, sum1):
        raws = ((raw00, raw01), (raw10, raw11))
        sums = (sum0, sum1)
        for ref in (*raws[0], *raws[1], *sums):
            pltpu.matmul_pop(ref)
        for c, copy in enumerate(copies):
            copy.wait()

            def tile(k, q):
                return slice((2 * k + q) * TILE, (2 * k + q + 1) * TILE)

            for k in (0, 1):
                for q in (0, 1):
                    at = slice(c * width + tile(k, q).start, c * width + tile(k, q).stop)
                    dosages = stage[c, :, tile(k, q)].astype(jnp.float32)
                    standard[c, :, tile(k, q)] = (
                        (dosages - mean[:, at]) * scaling[:, at]
                    ).astype(jnp.bfloat16)
                    pltpu.matmul_push_rhs(standard[c, :, tile(k, q)], k, q)
            for k in (0, 1):
                for q in (0, 1):
                    pltpu.matmul_acc_lhs(raws[q][k], left, load_staged_rhs=k)
                    pltpu.matmul_push_rhs(standard[c, :, tile(k, q)], k, q, transpose=True)
            for k in (0, 1):
                for q in (0, 1):
                    projected = pltpu.matmul_pop(raws[q][k]).astype(jnp.bfloat16)
                    pltpu.matmul_acc_lhs(sums[q], projected, load_staged_rhs=k)
        return pltpu.matmul_pop(sum0) + pltpu.matmul_pop(sum1)

    return pl.run_scoped(run, *acc)


def first_kernel(
    dosage, freq_hbm, probes_hbm, send, stage, standard, freq, probes, sems, *, snp_count, probe_count, columns
):
    samples, width = dosage.shape
    rows = probes.shape[0]
    part = samples // (snp_count * probe_count)
    step = width // CHUNKS
    copies = [
        pltpu.make_async_copy(dosage.at[:, pl.ds(c * step, step)], stage.at[c], sems.at[c])
        for c in range(CHUNKS)
    ]
    small = [
        pltpu.make_async_copy(freq_hbm, freq, sems.at[CHUNKS]),
        pltpu.make_async_copy(probes_hbm, probes, sems.at[CHUNKS + 1]),
    ]
    for copy in small + copies:
        copy.start()
    group = lax.axis_index("probe")
    row = lax.broadcasted_iota(jnp.int32, (snp_count * part, samples), 0)
    col = lax.broadcasted_iota(jnp.int32, (snp_count * part, samples), 1)
    owner = row // part
    wanted = owner * (part * probe_count) + group * part + (row - owner * part)
    pick = jnp.where(col == wanted, 1.0, 0.0).astype(jnp.bfloat16)
    for copy in small:
        copy.wait()
    signs = probes[...]
    blank = jnp.zeros((-(rows + pick.shape[0]) % 16, samples), jnp.bfloat16)
    left = jnp.concatenate([signs, pick, blank], axis=0)
    mean = 2.0 * freq[...]
    scaling = lax.rsqrt(mean * (1.0 - 0.5 * mean))
    if samples == TILE and step == 4 * TILE:
        total = tiled_products(left, mean, scaling, copies, stage, standard)
    else:
        total = jnp.zeros((left.shape[0], samples), jnp.float32)
        for c in range(CHUNKS):
            at = slice(c * step, (c + 1) * step)
            copies[c].wait()
            standard[c] = ((stage[c].astype(jnp.float32) - mean[:, at]) * scaling[:, at]).astype(
                jnp.bfloat16
            )
            projected = jnp.dot(left, standard[c], preferred_element_type=jnp.float32)
            total = total + lax.dot_general(
                projected.astype(jnp.bfloat16),
                standard[c],
                ACROSS,
                preferred_element_type=jnp.float32,
            )
    total = total * (1.0 / columns)
    exact = signs.astype(jnp.float32) * total[:rows]
    signed = exact.astype(jnp.bfloat16)
    rest = (exact - signed.astype(jnp.float32)).astype(jnp.bfloat16)
    kinship = total[rows:].astype(jnp.bfloat16)
    half = samples // 2
    for i in range(snp_count):
        block = jnp.concatenate([signed, rest, kinship[i * part : (i + 1) * part]], axis=0)
        for q in range(probe_count):
            send[q * snp_count + i] = block[:, (q % 2) * half : (q % 2 + 1) * half]


def sum_kernel(got, share, own, sums, *, snp_count, probe_count, rows):
    part = got.shape[1] - 2 * rows
    owned = part * probe_count
    group = lax.axis_index("probe")
    partner = group + 1 - 2 * (group % 2)
    first = jnp.zeros((rows, got.shape[2]), jnp.float32)
    second = first
    for q in range(probe_count):
        summed = got[q * snp_count].astype(jnp.float32)
        for j in range(1, snp_count):
            summed = summed + got[q * snp_count + j].astype(jnp.float32)
        signed = summed[:rows] + summed[rows : 2 * rows]
        sums[q] = signed
        share[q * part : (q + 1) * part] = summed[2 * rows :]
        first = first + signed
        second = second + signed.astype(jnp.bfloat16).astype(jnp.float32) * signed
    share[owned : owned + rows] = first
    share[owned + rows : owned + 2 * rows] = second
    share[owned + 2 * rows :] = sums[partner]
    own[...] = sums[group]


def last_kernel(share, other, own, probes, kin_twice, forms, estimates, *, probe_count):
    rows, samples = probes.shape
    half = samples // 2
    owned = share.shape[0] - 3 * rows
    low_half = lax.axis_index("probe") % 2 == 0
    scale = 1.0 / samples
    mean = scale / (rows * probe_count)
    ends = share[owned : owned + 2 * rows] + other[owned : owned + 2 * rows]
    lane = lax.broadcasted_iota(jnp.int32, (1, 2), 1)
    estimates[...] = jnp.where(lane == 0, jnp.sum(ends[:rows]), jnp.sum(ends[rows:])) * mean
    signs = probes[...].astype(jnp.float32)
    signs_low = signs[:, :half]
    signs_high = signs[:, half:]
    first = jnp.zeros((rows, half), jnp.float32)
    second = first
    twice = jnp.zeros((rows, owned), jnp.float32)
    for signed, rest, sign in (
        (own[...], share, jnp.where(low_half, signs_low, signs_high)),
        (other[owned + 2 * rows :], other, jnp.where(low_half, signs_high, signs_low)),
    ):
        rounded = signed.astype(jnp.bfloat16).astype(jnp.float32)
        first = first + signed
        second = second + rounded * signed
        vectors = (sign * rounded).astype(jnp.bfloat16)
        kinship = rest[:owned]
        high = kinship.astype(jnp.bfloat16)
        low = (kinship - high.astype(jnp.float32)).astype(jnp.bfloat16)
        for piece in (high, low):
            twice = twice + lax.dot_general(
                vectors, piece, ACROSS, preferred_element_type=jnp.float32
            )
    kin_twice[...] = twice
    at = lax.broadcasted_iota(jnp.int32, (rows, rows), 0)
    on = at == lax.broadcasted_iota(jnp.int32, (rows, rows), 1)
    for k, form in enumerate((first, second)):
        total = jnp.sum(form, axis=1, keepdims=True) * scale
        forms[k : k + 1] = jnp.sum(jnp.where(on, total, 0.0), axis=0, keepdims=True)


def body(dosage, allele_freq, probes):
    snp_count = lax.axis_size("snp")
    probe_count = lax.axis_size("probe")
    samples, width = dosage.shape
    rows = probes.shape[0]
    devices = snp_count * probe_count
    part = samples // devices
    half = samples // 2
    owned = samples // snp_count
    vmem = pl.BlockSpec(memory_space=pltpu.VMEM)
    hbm = pl.BlockSpec(memory_space=pltpu.HBM)
    stay = functools.partial(pltpu.with_memory_space_constraint, memory_space=pltpu.HBM)
    params = pltpu.CompilerParams(vmem_limit_bytes=min(56 << 20, max(16 << 20, 16 * samples * width)))
    send = pl.pallas_call(
        functools.partial(
            first_kernel, snp_count=snp_count, probe_count=probe_count, columns=width * snp_count
        ),
        in_specs=[hbm, hbm, hbm],
        out_specs=vmem,
        out_shape=jax.ShapeDtypeStruct((devices, 2 * rows + part, half), jnp.bfloat16),
        scratch_shapes=[
            pltpu.VMEM((CHUNKS, samples, width // CHUNKS), jnp.bfloat16),
            pltpu.VMEM((CHUNKS, samples, width // CHUNKS), jnp.bfloat16),
            pltpu.VMEM((1, width), jnp.float32),
            pltpu.VMEM((rows, samples), jnp.bfloat16),
            pltpu.SemaphoreType.DMA((CHUNKS + 2,)),
        ],
        compiler_params=params,
        name="first",
    )(*(stay(x) for x in (dosage, allele_freq.reshape(1, width), probes)))
    got = lax.all_to_all(send, BOTH, 0, 0, tiled=True)
    share, own = pl.pallas_call(
        functools.partial(sum_kernel, snp_count=snp_count, probe_count=probe_count, rows=rows),
        in_specs=[vmem],
        out_specs=[vmem, vmem],
        out_shape=[
            jax.ShapeDtypeStruct((owned + 3 * rows, half), jnp.float32),
            jax.ShapeDtypeStruct((rows, half), jnp.float32),
        ],
        scratch_shapes=[pltpu.VMEM((probe_count, rows, half), jnp.float32)],
        compiler_params=params,
        name="sums",
    )(got)
    other = lax.ppermute(share, "probe", [(q, q ^ 1) for q in range(probe_count)])
    kin_twice, forms, estimates = pl.pallas_call(
        functools.partial(last_kernel, probe_count=probe_count),
        in_specs=[vmem, vmem, vmem, vmem],
        out_specs=[vmem, vmem, vmem],
        out_shape=[
            jax.ShapeDtypeStruct((rows, owned), jnp.float32),
            jax.ShapeDtypeStruct((2, rows), jnp.float32),
            jax.ShapeDtypeStruct((1, 2), jnp.float32),
        ],
        compiler_params=params,
        name="last",
    )(share, other, own, probes)
    return (kin_twice, forms, estimates.reshape(2))


def solution(mesh):
    placed = (P(None, "snp"), P("snp"), P("probe", None))
    return jax.shard_map(
        body,
        mesh=mesh,
        in_specs=placed,
        out_specs=(P("probe", "snp"), P(None, "probe"), P()),
        check_vma=False,
    )
```

```python
import functools

import jax
import jax.numpy as jnp
from jax import lax
from jax.experimental import pallas as pl
from jax.experimental.pallas import tpu as pltpu
from jax.sharding import PartitionSpec as P

BOTH = ("probe", "snp")
ACROSS = (((1,), (1,)), ((), ()))
CHUNKS = 2
TILE = 256


def tiled_products(left, mean, scaling, copies, stage, standard):
    height = left.shape[0]
    acc = [pltpu.ACC(q)((height, TILE), jnp.float32) for q in (0, 1) for _ in range(3)]
    width = stage.shape[2]

    def run(raw00, raw01, sum0, raw10, raw11, sum1):
        raws = ((raw00, raw01), (raw10, raw11))
        sums = (sum0, sum1)
        for ref in (*raws[0], *raws[1], *sums):
            pltpu.matmul_pop(ref)
        for c, copy in enumerate(copies):
            copy.wait()

            def tile(k, q):
                return slice((2 * k + q) * TILE, (2 * k + q + 1) * TILE)

            for k in (0, 1):
                for q in (0, 1):
                    at = slice(c * width + tile(k, q).start, c * width + tile(k, q).stop)
                    dosages = stage[c, :, tile(k, q)].astype(jnp.float32)
                    standard[c, :, tile(k, q)] = (
                        (dosages - mean[:, at]) * scaling[:, at]
                    ).astype(jnp.bfloat16)
                    pltpu.matmul_push_rhs(standard[c, :, tile(k, q)], k, q)
            for k in (0, 1):
                for q in (0, 1):
                    pltpu.matmul_acc_lhs(raws[q][k], left, load_staged_rhs=k)
                    pltpu.matmul_push_rhs(standard[c, :, tile(k, q)], k, q, transpose=True)
            for k in (0, 1):
                for q in (0, 1):
                    projected = pltpu.matmul_pop(raws[q][k]).astype(jnp.bfloat16)
                    pltpu.matmul_acc_lhs(sums[q], projected, load_staged_rhs=k)
        return pltpu.matmul_pop(sum0) + pltpu.matmul_pop(sum1)

    return pl.run_scoped(run, *acc)


def first_kernel(
    dosage, freq_hbm, probes_hbm, send, stage, standard, freq, probes, sems, *, snp_count, probe_count, columns
):
    samples, width = dosage.shape
    rows = probes.shape[0]
    part = samples // (snp_count * probe_count)
    step = width // CHUNKS
    copies = [
        pltpu.make_async_copy(dosage.at[:, pl.ds(c * step, step)], stage.at[c], sems.at[c])
        for c in range(CHUNKS)
    ]
    small = [
        pltpu.make_async_copy(freq_hbm, freq, sems.at[CHUNKS]),
        pltpu.make_async_copy(probes_hbm, probes, sems.at[CHUNKS + 1]),
    ]
    for copy in small + copies:
        copy.start()
    group = lax.axis_index("probe")
    row = lax.broadcasted_iota(jnp.int32, (snp_count * part, samples), 0)
    col = lax.broadcasted_iota(jnp.int32, (snp_count * part, samples), 1)
    owner = row // part
    wanted = owner * (part * probe_count) + group * part + (row - owner * part)
    pick = jnp.where(col == wanted, 1.0, 0.0).astype(jnp.bfloat16)
    for copy in small:
        copy.wait()
    signs = probes[...]
    blank = jnp.zeros((-(rows + pick.shape[0]) % 16, samples), jnp.bfloat16)
    left = jnp.concatenate([signs, pick, blank], axis=0)
    mean = 2.0 * freq[...]
    scaling = lax.rsqrt(mean * (1.0 - 0.5 * mean))
    if samples == TILE and step == 4 * TILE:
        total = tiled_products(left, mean, scaling, copies, stage, standard)
    else:
        total = jnp.zeros((left.shape[0], samples), jnp.float32)
        for c in range(CHUNKS):
            at = slice(c * step, (c + 1) * step)
            copies[c].wait()
            standard[c] = ((stage[c].astype(jnp.float32) - mean[:, at]) * scaling[:, at]).astype(
                jnp.bfloat16
            )
            projected = jnp.dot(left, standard[c], preferred_element_type=jnp.float32)
            total = total + lax.dot_general(
                projected.astype(jnp.bfloat16),
                standard[c],
                ACROSS,
                preferred_element_type=jnp.float32,
            )
    total = total * (1.0 / columns)
    signed = (signs.astype(jnp.float32) * total[:rows]).astype(jnp.bfloat16)
    kinship = total[rows:].astype(jnp.bfloat16)
    half = samples // 2
    for i in range(snp_count):
        block = jnp.concatenate([signed, kinship[i * part : (i + 1) * part]], axis=0)
        for q in range(probe_count):
            send[q * snp_count + i] = block[:, (q % 2) * half : (q % 2 + 1) * half]


def sum_kernel(got, share, own, sums, *, snp_count, probe_count, rows):
    part = got.shape[1] - rows
    owned = part * probe_count
    group = lax.axis_index("probe")
    partner = group + 1 - 2 * (group % 2)
    first = jnp.zeros((rows, got.shape[2]), jnp.float32)
    second = first
    for q in range(probe_count):
        summed = got[q * snp_count].astype(jnp.float32)
        for j in range(1, snp_count):
            summed = summed + got[q * snp_count + j].astype(jnp.float32)
        signed = summed[:rows]
        sums[q] = signed
        share[q * part : (q + 1) * part] = summed[rows:]
        first = first + signed
        second = second + signed.astype(jnp.bfloat16).astype(jnp.float32) * signed
    share[owned : owned + rows] = first
    share[owned + rows : owned + 2 * rows] = second
    share[owned + 2 * rows :] = sums[partner]
    own[...] = sums[group]


def half_products(signed, kinship, sign):
    rounded = signed.astype(jnp.bfloat16).astype(jnp.float32)
    vectors = (sign * rounded).astype(jnp.bfloat16)
    high = kinship.astype(jnp.bfloat16)
    low = (kinship - high.astype(jnp.float32)).astype(jnp.bfloat16)
    twice = lax.dot_general(
        vectors, high, ACROSS, preferred_element_type=jnp.float32
    ) + lax.dot_general(vectors, low, ACROSS, preferred_element_type=jnp.float32)
    return twice, rounded * signed


def half_signs(probes, own):
    half = probes.shape[1] // 2
    signs = probes[...].astype(jnp.float32)
    low_half = lax.axis_index("probe") % 2 == 0
    return jnp.where(low_half == own, signs[:, :half], signs[:, half:])


def near_kernel(share, own, probes, near_twice, near_second):
    owned = near_twice.shape[1]
    near_twice[...], near_second[...] = half_products(
        own[...], share[:owned], half_signs(probes, True)
    )


def last_kernel(
    share, other, own, near_twice, near_second, probes, kin_twice, forms, estimates, *, probe_count
):
    rows, samples = probes.shape
    owned = near_twice.shape[1]
    scale = 1.0 / samples
    mean = scale / (rows * probe_count)
    ends = share[owned : owned + 2 * rows] + other[owned : owned + 2 * rows]
    lane = lax.broadcasted_iota(jnp.int32, (1, 2), 1)
    estimates[...] = jnp.where(lane == 0, jnp.sum(ends[:rows]), jnp.sum(ends[rows:])) * mean
    signed = other[owned + 2 * rows :]
    twice, second = half_products(signed, other[:owned], half_signs(probes, False))
    kin_twice[...] = near_twice[...] + twice
    at = lax.broadcasted_iota(jnp.int32, (rows, rows), 0)
    on = at == lax.broadcasted_iota(jnp.int32, (rows, rows), 1)
    for k, form in enumerate((own[...] + signed, near_second[...] + second)):
        total = jnp.sum(form, axis=1, keepdims=True) * scale
        forms[k : k + 1] = jnp.sum(jnp.where(on, total, 0.0), axis=0, keepdims=True)


def body(dosage, allele_freq, probes):
    snp_count = lax.axis_size("snp")
    probe_count = lax.axis_size("probe")
    samples, width = dosage.shape
    rows = probes.shape[0]
    devices = snp_count * probe_count
    part = samples // devices
    half = samples // 2
    owned = samples // snp_count
    vmem = pl.BlockSpec(memory_space=pltpu.VMEM)
    hbm = pl.BlockSpec(memory_space=pltpu.HBM)
    stay = functools.partial(pltpu.with_memory_space_constraint, memory_space=pltpu.HBM)
    params = pltpu.CompilerParams(vmem_limit_bytes=min(56 << 20, max(16 << 20, 16 * samples * width)))
    send = pl.pallas_call(
        functools.partial(
            first_kernel, snp_count=snp_count, probe_count=probe_count, columns=width * snp_count
        ),
        in_specs=[hbm, hbm, hbm],
        out_specs=vmem,
        out_shape=jax.ShapeDtypeStruct((devices, rows + part, half), jnp.bfloat16),
        scratch_shapes=[
            pltpu.VMEM((CHUNKS, samples, width // CHUNKS), jnp.bfloat16),
            pltpu.VMEM((CHUNKS, samples, width // CHUNKS), jnp.bfloat16),
            pltpu.VMEM((1, width), jnp.float32),
            pltpu.VMEM((rows, samples), jnp.bfloat16),
            pltpu.SemaphoreType.DMA((CHUNKS + 2,)),
        ],
        compiler_params=params,
        name="first",
    )(*(stay(x) for x in (dosage, allele_freq.reshape(1, width), probes)))
    got = lax.all_to_all(send, BOTH, 0, 0, tiled=True)
    share, own = pl.pallas_call(
        functools.partial(sum_kernel, snp_count=snp_count, probe_count=probe_count, rows=rows),
        in_specs=[vmem],
        out_specs=[vmem, vmem],
        out_shape=[
            jax.ShapeDtypeStruct((owned + 3 * rows, half), jnp.float32),
            jax.ShapeDtypeStruct((rows, half), jnp.float32),
        ],
        scratch_shapes=[pltpu.VMEM((probe_count, rows, half), jnp.float32)],
        compiler_params=params,
        name="sums",
    )(got)
    other = lax.ppermute(share, "probe", [(q, q ^ 1) for q in range(probe_count)])
    near = pl.pallas_call(
        near_kernel,
        in_specs=[vmem, vmem, vmem],
        out_specs=[vmem, vmem],
        out_shape=[
            jax.ShapeDtypeStruct((rows, owned), jnp.float32),
            jax.ShapeDtypeStruct((rows, half), jnp.float32),
        ],
        compiler_params=params,
        name="near",
    )(share, own, probes)
    kin_twice, forms, estimates = pl.pallas_call(
        functools.partial(last_kernel, probe_count=probe_count),
        in_specs=[vmem] * 6,
        out_specs=[vmem, vmem, vmem],
        out_shape=[
            jax.ShapeDtypeStruct((rows, owned), jnp.float32),
            jax.ShapeDtypeStruct((2, rows), jnp.float32),
            jax.ShapeDtypeStruct((1, 2), jnp.float32),
        ],
        compiler_params=params,
        name="last",
    )(share, other, own, *near, probes)
    return (kin_twice, forms, estimates.reshape(2))


def solution(mesh):
    placed = (P(None, "snp"), P("snp"), P("probe", None))
    return jax.shard_map(
        body,
        mesh=mesh,
        in_specs=placed,
        out_specs=(P("probe", "snp"), P(None, "probe"), P()),
        check_vma=False,
    )
```

```python
import functools

import jax
import jax.numpy as jnp
from jax import lax
from jax.experimental import pallas as pl
from jax.experimental.pallas import tpu as pltpu
from jax.sharding import PartitionSpec as P

BOTH = ("probe", "snp")
ACROSS = (((1,), (1,)), ((), ()))
CHUNKS = 2
TILE = 256


def tiled_products(left, mean, scaling, copies, stage, standard):
    height = left.shape[0]
    acc = [pltpu.ACC(q)((height, TILE), jnp.float32) for q in (0, 1) for _ in range(3)]
    width = stage.shape[2]

    def run(raw00, raw01, sum0, raw10, raw11, sum1):
        raws = ((raw00, raw01), (raw10, raw11))
        sums = (sum0, sum1)
        for ref in (*raws[0], *raws[1], *sums):
            pltpu.matmul_pop(ref)
        for c, copy in enumerate(copies):
            copy.wait()

            def tile(k, q):
                return slice((2 * k + q) * TILE, (2 * k + q + 1) * TILE)

            for k in (0, 1):
                for q in (0, 1):
                    at = slice(c * width + tile(k, q).start, c * width + tile(k, q).stop)
                    dosages = stage[c, :, tile(k, q)].astype(jnp.float32)
                    standard[c, :, tile(k, q)] = (
                        (dosages - mean[:, at]) * scaling[:, at]
                    ).astype(jnp.bfloat16)
                    pltpu.matmul_push_rhs(standard[c, :, tile(k, q)], k, q)
                for q in (0, 1):
                    pltpu.matmul_acc_lhs(raws[q][k], left, load_staged_rhs=k)
                    pltpu.matmul_push_rhs(standard[c, :, tile(k, q)], k, q, transpose=True)
            for k in (0, 1):
                for q in (0, 1):
                    projected = pltpu.matmul_pop(raws[q][k]).astype(jnp.bfloat16)
                    pltpu.matmul_acc_lhs(sums[q], projected, load_staged_rhs=k)
        return pltpu.matmul_pop(sum0) + pltpu.matmul_pop(sum1)

    return pl.run_scoped(run, *acc)


def first_kernel(
    dosage, freq_hbm, probes_hbm, send, stage, standard, freq, probes, sems, *, snp_count, probe_count, columns
):
    samples, width = dosage.shape
    rows = probes.shape[0]
    part = samples // (snp_count * probe_count)
    step = width // CHUNKS
    copies = [
        pltpu.make_async_copy(dosage.at[:, pl.ds(c * step, step)], stage.at[c], sems.at[c])
        for c in range(CHUNKS)
    ]
    small = [
        pltpu.make_async_copy(freq_hbm, freq, sems.at[CHUNKS]),
        pltpu.make_async_copy(probes_hbm, probes, sems.at[CHUNKS + 1]),
    ]
    for copy in small + copies:
        copy.start()
    group = lax.axis_index("probe")
    row = lax.broadcasted_iota(jnp.int32, (snp_count * part, samples), 0)
    col = lax.broadcasted_iota(jnp.int32, (snp_count * part, samples), 1)
    owner = row // part
    wanted = owner * (part * probe_count) + group * part + (row - owner * part)
    pick = jnp.where(col == wanted, 1.0, 0.0).astype(jnp.bfloat16)
    for copy in small:
        copy.wait()
    signs = probes[...]
    blank = jnp.zeros((-(rows + pick.shape[0]) % 16, samples), jnp.bfloat16)
    left = jnp.concatenate([signs, pick, blank], axis=0)
    mean = 2.0 * freq[...]
    scaling = lax.rsqrt(mean * (1.0 - 0.5 * mean))
    if samples == TILE and step == 4 * TILE:
        total = tiled_products(left, mean, scaling, copies, stage, standard)
    else:
        total = jnp.zeros((left.shape[0], samples), jnp.float32)
        for c in range(CHUNKS):
            at = slice(c * step, (c + 1) * step)
            copies[c].wait()
            standard[c] = ((stage[c].astype(jnp.float32) - mean[:, at]) * scaling[:, at]).astype(
                jnp.bfloat16
            )
            projected = jnp.dot(left, standard[c], preferred_element_type=jnp.float32)
            total = total + lax.dot_general(
                projected.astype(jnp.bfloat16),
                standard[c],
                ACROSS,
                preferred_element_type=jnp.float32,
            )
    total = total * (1.0 / columns)
    signed = (signs.astype(jnp.float32) * total[:rows]).astype(jnp.bfloat16)
    kinship = total[rows:].astype(jnp.bfloat16)
    half = samples // 2
    for i in range(snp_count):
        block = jnp.concatenate([signed, kinship[i * part : (i + 1) * part]], axis=0)
        for q in range(probe_count):
            send[q * snp_count + i] = block[:, (q % 2) * half : (q % 2 + 1) * half]


def sum_kernel(got, share, own, sums, *, snp_count, probe_count, rows):
    part = got.shape[1] - rows
    owned = part * probe_count
    group = lax.axis_index("probe")
    partner = group + 1 - 2 * (group % 2)
    first = jnp.zeros((rows, got.shape[2]), jnp.float32)
    second = first
    for q in range(probe_count):
        summed = got[q * snp_count].astype(jnp.float32)
        for j in range(1, snp_count):
            summed = summed + got[q * snp_count + j].astype(jnp.float32)
        signed = summed[:rows]
        sums[q] = signed
        share[q * part : (q + 1) * part] = summed[rows:]
        first = first + signed
        second = second + signed.astype(jnp.bfloat16).astype(jnp.float32) * signed
    share[owned : owned + rows] = first
    share[owned + rows : owned + 2 * rows] = second
    share[owned + 2 * rows :] = sums[partner]
    own[...] = sums[group]


def last_kernel(share, other, own, probes, kin_twice, forms, estimates, *, probe_count):
    rows, samples = probes.shape
    half = samples // 2
    owned = share.shape[0] - 3 * rows
    low_half = lax.axis_index("probe") % 2 == 0
    scale = 1.0 / samples
    mean = scale / (rows * probe_count)
    ends = share[owned : owned + 2 * rows] + other[owned : owned + 2 * rows]
    lane = lax.broadcasted_iota(jnp.int32, (1, 2), 1)
    estimates[...] = jnp.where(lane == 0, jnp.sum(ends[:rows]), jnp.sum(ends[rows:])) * mean
    signs = probes[...].astype(jnp.float32)
    signs_low = signs[:, :half]
    signs_high = signs[:, half:]
    first = jnp.zeros((rows, half), jnp.float32)
    second = first
    twice = jnp.zeros((rows, owned), jnp.float32)
    for signed, rest, sign in (
        (own[...], share, jnp.where(low_half, signs_low, signs_high)),
        (other[owned + 2 * rows :], other, jnp.where(low_half, signs_high, signs_low)),
    ):
        rounded = signed.astype(jnp.bfloat16).astype(jnp.float32)
        first = first + signed
        second = second + rounded * signed
        vectors = (sign * rounded).astype(jnp.bfloat16)
        kinship = rest[:owned]
        high = kinship.astype(jnp.bfloat16)
        low = (kinship - high.astype(jnp.float32)).astype(jnp.bfloat16)
        for piece in (high, low):
            twice = twice + lax.dot_general(
                vectors, piece, ACROSS, preferred_element_type=jnp.float32
            )
    kin_twice[...] = twice
    at = lax.broadcasted_iota(jnp.int32, (rows, rows), 0)
    on = at == lax.broadcasted_iota(jnp.int32, (rows, rows), 1)
    for k, form in enumerate((first, second)):
        total = jnp.sum(form, axis=1, keepdims=True) * scale
        forms[k : k + 1] = jnp.sum(jnp.where(on, total, 0.0), axis=0, keepdims=True)


def body(dosage, allele_freq, probes):
    snp_count = lax.axis_size("snp")
    probe_count = lax.axis_size("probe")
    samples, width = dosage.shape
    rows = probes.shape[0]
    devices = snp_count * probe_count
    part = samples // devices
    half = samples // 2
    owned = samples // snp_count
    vmem = pl.BlockSpec(memory_space=pltpu.VMEM)
    hbm = pl.BlockSpec(memory_space=pltpu.HBM)
    stay = functools.partial(pltpu.with_memory_space_constraint, memory_space=pltpu.HBM)
    params = pltpu.CompilerParams(vmem_limit_bytes=min(56 << 20, max(16 << 20, 16 * samples * width)))
    send = pl.pallas_call(
        functools.partial(
            first_kernel, snp_count=snp_count, probe_count=probe_count, columns=width * snp_count
        ),
        in_specs=[hbm, hbm, hbm],
        out_specs=vmem,
        out_shape=jax.ShapeDtypeStruct((devices, rows + part, half), jnp.bfloat16),
        scratch_shapes=[
            pltpu.VMEM((CHUNKS, samples, width // CHUNKS), jnp.bfloat16),
            pltpu.VMEM((CHUNKS, samples, width // CHUNKS), jnp.bfloat16),
            pltpu.VMEM((1, width), jnp.float32),
            pltpu.VMEM((rows, samples), jnp.bfloat16),
            pltpu.SemaphoreType.DMA((CHUNKS + 2,)),
        ],
        compiler_params=params,
        name="first",
    )(*(stay(x) for x in (dosage, allele_freq.reshape(1, width), probes)))
    got = lax.all_to_all(send, BOTH, 0, 0, tiled=True)
    share, own = pl.pallas_call(
        functools.partial(sum_kernel, snp_count=snp_count, probe_count=probe_count, rows=rows),
        in_specs=[vmem],
        out_specs=[vmem, vmem],
        out_shape=[
            jax.ShapeDtypeStruct((owned + 3 * rows, half), jnp.float32),
            jax.ShapeDtypeStruct((rows, half), jnp.float32),
        ],
        scratch_shapes=[pltpu.VMEM((probe_count, rows, half), jnp.float32)],
        compiler_params=params,
        name="sums",
    )(got)
    other = lax.ppermute(share, "probe", [(q, q ^ 1) for q in range(probe_count)])
    kin_twice, forms, estimates = pl.pallas_call(
        functools.partial(last_kernel, probe_count=probe_count),
        in_specs=[vmem, vmem, vmem, vmem],
        out_specs=[vmem, vmem, vmem],
        out_shape=[
            jax.ShapeDtypeStruct((rows, owned), jnp.float32),
            jax.ShapeDtypeStruct((2, rows), jnp.float32),
            jax.ShapeDtypeStruct((1, 2), jnp.float32),
        ],
        compiler_params=params,
        name="last",
    )(share, other, own, probes)
    return (kin_twice, forms, estimates.reshape(2))


def solution(mesh):
    placed = (P(None, "snp"), P("snp"), P("probe", None))
    return jax.shard_map(
        body,
        mesh=mesh,
        in_specs=placed,
        out_specs=(P("probe", "snp"), P(None, "probe"), P()),
        check_vma=False,
    )
```
